32 devices in a mesh: tm: 2 (over x), py: 4 (over z), pz: 4 (over y, core).
Axes of the slice: x: 2, y: 2, z: 4, core: 2. Of those that a mesh axis runs over, the one named last changes fastest.
Arguments:
- state_old: float32 [2, 4, 128, 128, 128], P('tm', None, 'py', 'pz'), may hold values from -6 to 6
Outputs:
- new_states: float32 [2, 4, 128, 128, 128], P('tm', None, 'py', 'pz')
The draws below stay inside these ranges and needn't reach their ends.
All inputs are finite; a program needn't handle non-finite values.
Results may differ from the reference program's by a relative error of at most 0.00017.
Values sent between devices are 32-bit elements; how exact they have to be, the bound alone decides.
No kernel may reach another device: no remote copies, remote signals or barrier semaphores. Data moves between devices by JAX's collectives and lax.ppermute only.
A program may use at most 128 MiB of HBM per device.

```python
import jax
import jax.numpy as jnp
from jax import lax

N = 128
KMAX = 42
KCO = 21
SLICES = 2


def level_of(own_key, shape, split, low, top_value):
    level, own = 1.0, jax.random.fold_in(own_key, 6)
    for dim, parts in split:
        draws = jnp.exp(jax.random.uniform(jax.random.fold_in(own, dim), (parts,), jnp.float32, low / len(split), top_value / len(split)))
        level = level * jnp.repeat(draws, shape[dim] // parts).reshape([-1 if axis == dim else 1 for axis in range(len(shape))])
    return level


def normal_values(rng, dims, spread, most, shards=(), held_as=jnp.bfloat16):
    level = level_of(rng, dims, shards, -0.22, 0.18) if shards else 1.0
    entries = jax.random.normal(rng, dims, jnp.float32) * spread * level
    return jnp.minimum(jnp.maximum(entries, -most), most).astype(held_as)


def setup_inputs(seed: int = 0) -> dict:
    keys = jax.random.split(jax.random.key(seed), 2)
    state_old = normal_values(keys[0], (SLICES, 4, N, N, N), 1.0, 6.0, ((0, 2), (2, 4), (3, 4)), jnp.float32)
    return dict(state_old=state_old)


time_step = 0.01
coriolis = 6.0
buoyancy_square = 100.0
viscosity = 0.001
diffusivity = 0.001


def wave_grid():
    wave_x = jnp.arange(KMAX + 1).astype(jnp.float32)[:, None, None]
    centred = (jnp.arange(2 * KMAX + 1) - KMAX).astype(jnp.float32)
    return wave_x, centred[None, :, None], centred[None, None, :]


def synthesis(modes):
    weight = jnp.where(jnp.arange(KMAX + 1) == 0, 1.0, 2.0).astype(jnp.float32)
    weighted = modes * weight[None, :, None, None]
    padded = jnp.pad(weighted, ((0, 0), (0, N - KMAX - 1), (0, N - 2 * KMAX - 1), (0, N - 2 * KMAX - 1)))
    padded = jnp.roll(padded, (-KMAX, -KMAX), axis=(2, 3))
    return jnp.real(jnp.fft.ifftn(padded, axes=(1, 2, 3))) * (N ** 1.5)


def analysis(fields):
    spectrum = jnp.fft.fftn(fields, axes=(1, 2, 3)) * (N ** -1.5)
    rolled = jnp.roll(spectrum, (KMAX, KMAX), axis=(2, 3))
    return rolled[:, :KMAX + 1, :2 * KMAX + 1, :2 * KMAX + 1]


def project(velocity):
    wave_x, wave_y, wave_z = wave_grid()
    square = wave_x ** 2 + wave_y ** 2 + wave_z ** 2
    along = (wave_x * velocity[0] + wave_y * velocity[1] + wave_z * velocity[2]) / jnp.maximum(square, 1.0)
    return velocity[0] - wave_x * along, velocity[1] - wave_y * along, velocity[2] - wave_z * along


def rate(state):
    wave_x, wave_y, wave_z = wave_grid()
    square = wave_x ** 2 + wave_y ** 2 + wave_z ** 2
    spin = 1j * jnp.stack([wave_y * state[2] - wave_z * state[1],
                           wave_z * state[0] - wave_x * state[2],
                           wave_x * state[1] - wave_y * state[0]])
    fields = synthesis(jnp.concatenate([state, spin]))
    speed_x, speed_y, speed_z, lift = fields[0], fields[1], fields[2], fields[3]
    spin_x, spin_y, spin_z = fields[4], fields[5], fields[6]
    products = jnp.stack([speed_y * spin_z - speed_z * spin_y,
                          speed_z * spin_x - speed_x * spin_z,
                          speed_x * spin_y - speed_y * spin_x,
                          speed_x * lift, speed_y * lift, speed_z * lift])
    modes = analysis(products)
    pushed = project((modes[0] + coriolis * state[1], modes[1] - coriolis * state[0], modes[2] + state[3]))
    lift_rate = (-1j * (wave_x * modes[3] + wave_y * modes[4] + wave_z * modes[5])
                 - buoyancy_square * state[2] - diffusivity * square * state[3])
    return jnp.stack([pushed[0] - viscosity * square * state[0],
                      pushed[1] - viscosity * square * state[1],
                      pushed[2] - viscosity * square * state[2],
                      lift_rate])


def fine_step(state):
    return state + time_step * rate(state)


def linear(state):
    wave_x, wave_y, wave_z = wave_grid()
    square = wave_x ** 2 + wave_y ** 2 + wave_z ** 2
    pushed = project((coriolis * state[1], -coriolis * state[0], state[3]))
    return jnp.stack([pushed[0] - viscosity * square * state[0],
                      pushed[1] - viscosity * square * state[1],
                      pushed[2] - viscosity * square * state[2],
                      -buoyancy_square * state[2] - diffusivity * square * state[3]])


def propagate(state):
    for half_step in range(2):
        anchor = state
        for order in (4.0, 3.0, 2.0, 1.0):
            state = anchor + (0.5 * time_step / order) * linear(state)
    return state


def reference(state_old):
    def one_slice(fields):
        physical = jnp.transpose(fields, (0, 3, 1, 2))
        start = analysis(physical)
        velocity = project((start[0], start[1], start[2]))
        start = jnp.concatenate([jnp.stack(velocity), start[3:]])
        return start, fine_step(start)

    starts, fines = lax.map(one_slice, state_old)
    wave_x, wave_y, wave_z = wave_grid()
    inside = (wave_x <= KCO) & (jnp.abs(wave_y) <= KCO) & (jnp.abs(wave_z) <= KCO)
    keep = inside.astype(jnp.float32)
    outputs = []
    carry = keep * fines[0]
    for index in range(SLICES):
        if index > 0:
            carry = keep * fines[index] - keep * propagate(starts[index]) + keep * propagate(carry)
        merged = jnp.where(inside, carry, fines[index])
        outputs.append(jnp.transpose(synthesis(merged), (0, 2, 3, 1)))
    return jnp.stack(outputs)
```

```python
import functools

import jax
import jax.numpy as jnp
import numpy as np
from jax import lax
from jax.experimental import pallas as pl
from jax.experimental.pallas import tpu as pltpu
from jax.sharding import PartitionSpec as P

KMAX = 42
KCO = 21

time_step = 0.01
coriolis = 6.0
buoyancy_square = 100.0
viscosity = 0.001
diffusivity = 0.001

LANES = 128
PAIRS = ("py", "pz")
VMEM_LIMIT = 56 * 1024 * 1024


def up_to(value, step):
    return (value + step - 1) // step * step


class Plan:
    def __init__(self, shape, across_t, across_y, across_z):
        _, self.fields, self.rows_y, self.rows_z, self.extent = shape
        self.across_t, self.across_y, self.across_z = across_t, across_y, across_z
        self.joint = across_y * across_z
        self.slots = up_to(KMAX + 1, self.joint) // self.joint
        self.coarse_slots = up_to(KCO + 1, self.joint) // self.joint
        self.group = LANES // self.rows_z
        self.tiles = self.rows_y * self.rows_z // LANES
        self.waves = 2 * KMAX + 1
        self.wave_rows = up_to(self.waves, 8)
        self.coarse_rows = up_to(2 * KCO + 1, 8)
        assert self.extent == LANES and self.extent > 3 * KMAX
        assert self.group == self.across_z and self.tiles == 8
        assert 2 * KCO + 1 <= LANES // 2 <= self.waves <= LANES
        inner = list(range(-KCO, KCO + 1))
        outer = [k for k in range(-KMAX, KMAX + 1) if abs(k) > KCO]
        self.order = np.array(inner + outer)

    def angle(self, waves, cells):
        return 2.0 * np.pi / self.extent * ((waves[:, None] * cells[None, :]) % self.extent)

    def first(self):
        cells = np.arange(self.extent)
        waves = np.arange(self.slots * self.joint)
        inside = (waves <= KMAX)[:, None] * self.extent**-0.5
        weight = np.where(waves == 0, 1.0, 2.0)[:, None] * inside
        angle = self.angle(waves, cells)
        both = np.stack([np.cos(angle), -np.sin(angle)])

        def rows(table):
            table = table.reshape(2, self.slots, self.joint, self.extent)
            return table.transpose(1, 0, 2, 3).reshape(-1, self.extent)

        return rows(both * inside), rows(both * weight).T

    def other(self, size, cells):
        angle = self.angle(self.order, cells)
        cosine = np.zeros((size, len(cells)))
        sine = np.zeros((size, len(cells)))
        cosine[: self.waves] = np.cos(angle) * self.extent**-0.5
        sine[: self.waves] = np.sin(angle) * self.extent**-0.5
        return cosine, sine

    def along_z(self):
        cosine, sine = self.other(LANES, np.arange(self.extent))
        fore = np.block([[cosine.T, -sine.T], [sine.T, cosine.T]])
        back = np.block([[cosine, sine], [-sine, cosine]])
        return fore, back

    def along_y(self):
        cell = np.arange(self.extent).reshape(self.across_y, self.tiles, self.group)
        cosine, sine = self.other(self.wave_rows, cell.transpose(0, 2, 1).reshape(-1))
        fore = np.block([[cosine, sine], [-sine, cosine]])
        back = np.block([[cosine.T, -sine.T], [sine.T, cosine.T]])
        return fore, back

    def wave_tables(self):
        wave_y = np.zeros((self.wave_rows, LANES), np.float32)
        wave_y[: self.waves] = self.order[:, None]
        wave_z = np.zeros((self.wave_rows, LANES), np.float32)
        wave_z[:, : self.waves] = self.order[None, :]
        packed_z = np.tile(self.order[: LANES // 2], 2)
        packed_z = np.broadcast_to(packed_z, (self.coarse_rows, LANES))
        return wave_y, wave_z, packed_z.astype(np.float32)


def split_table(table):
    high = np.asarray(table, np.float32).astype(jnp.bfloat16)
    low = (table - high.astype(np.float64)).astype(np.float32).astype(jnp.bfloat16)
    return high, low


def split(values):
    high = values.astype(jnp.bfloat16)
    low = (values - high.astype(jnp.float32)).astype(jnp.bfloat16)
    return high, low


def dot(left, right, dims=((1,), (0,))):
    return lax.dot_general(left, right, (dims, ((), ())), preferred_element_type=jnp.float32)


def from_left(table, values, dims=((1,), (0,))):
    high, low = split(values)
    table_high, table_low = table[0][...], table[1][...]
    return dot(table_high, high, dims) + (dot(table_high, low, dims) + dot(table_low, high, dims))


def from_right(values, table):
    high, low = split(values)
    table_high, table_low = table[0][...], table[1][...]
    return dot(high, table_high) + (dot(low, table_high) + dot(high, table_low))


def swap_lanes(tiles, width):
    tiles = list(tiles)
    count = len(tiles)
    assert count * width == LANES
    lane = lax.broadcasted_iota(jnp.int32, tiles[0].shape, 1)
    step = count // 2
    while step:
        reach = step * width
        low = (lane // reach) % 2 == 0
        for i in range(count):
            if (i // step) % 2 == 0:
                a, b = tiles[i], tiles[i + step]
                tiles[i] = jnp.where(low, a, pltpu.roll(b, reach, 1))
                tiles[i + step] = jnp.where(low, pltpu.roll(a, LANES - reach, 1), b)
        step //= 2
    return tiles


def arrived_planes(plan, ref, count):
    tiles = plan.tiles
    planes = []
    for f in range(count):
        for c in range(2):
            rows = []
            for p in range(plan.across_y):
                rows.append([ref[p * plan.across_z + q, f, c * tiles : (c + 1) * tiles, :] for q in range(plan.across_z)])
            per_source = [jnp.concatenate([r[q] for r in rows], axis=0) for q in range(plan.across_z)]
            swapped = swap_lanes(per_source, plan.rows_z)
            pieces = []
            for p in range(plan.across_y):
                for g in range(plan.group):
                    pieces.append(swapped[g][p * tiles : (p + 1) * tiles])
            planes.append(jnp.concatenate(pieces, axis=0))
    return planes


def to_waves(plan, ref, count, fore_y, fore_z):
    planes = arrived_planes(plan, ref, count)
    extent = plan.extent
    stacked = jnp.concatenate(
        [jnp.concatenate([planes[2 * f], planes[2 * f + 1]], axis=1) for f in range(count)], axis=0
    )
    along_z = from_right(stacked, fore_z)
    beside = jnp.concatenate(
        [
            jnp.concatenate(
                [along_z[f * extent : (f + 1) * extent, c * LANES : (c + 1) * LANES] for c in range(2)], axis=0
            )
            for f in range(count)
        ],
        axis=1,
    )
    along_y = from_left(fore_y, beside)
    rows = plan.wave_rows
    return [
        [along_y[c * rows : (c + 1) * rows, f * LANES : (f + 1) * LANES] for c in range(2)]
        for f in range(count)
    ]


def send_waves(plan, modes, ref, back_y, back_z):
    count, extent, tiles = len(modes), plan.extent, plan.tiles
    beside = jnp.concatenate([jnp.concatenate(parts, axis=0) for parts in modes], axis=1)
    along_y = from_left(back_y, beside)
    stacked = jnp.concatenate(
        [
            jnp.concatenate(
                [along_y[c * extent : (c + 1) * extent, f * LANES : (f + 1) * LANES] for c in range(2)], axis=1
            )
            for f in range(count)
        ],
        axis=0,
    )
    along_z = from_right(stacked, back_z)
    for f in range(count):
        for c in range(2):
            plane = along_z[f * extent : (f + 1) * extent, c * LANES : (c + 1) * LANES]
            groups = []
            for g in range(plan.group):
                rows = [(p * plan.group + g) * tiles for p in range(plan.across_y)]
                groups.append(jnp.concatenate([plane[r : r + tiles] for r in rows], axis=0))
            swapped = swap_lanes(groups, plan.rows_z)
            for p in range(plan.across_y):
                for q in range(plan.across_z):
                    ref[p * plan.across_z + q, f, c * tiles : (c + 1) * tiles, :] = swapped[q][
                        p * tiles : (p + 1) * tiles
                    ]


def store_first(plan, ref, values, field, count, tile):
    block = 2 * plan.slots * plan.tiles
    for i in range(2 * plan.slots):
        rows = pl.ds(field * block + i * plan.tiles + tile, plan.joint, stride=count * block)
        ref[rows, :] = values[i * plan.joint : (i + 1) * plan.joint]


def load_first(plan, ref, field, count, tile):
    block = 2 * plan.slots * plan.tiles
    return jnp.concatenate(
        [
            ref[pl.ds(field * block + i * plan.tiles + tile, plan.joint, stride=count * block), :]
            for i in range(2 * plan.slots)
        ],
        axis=0,
    )


def begin_kernel(plan, state, fore_high, fore_low, out):
    fore = (fore_high, fore_low)
    count = plan.fields
    for f in range(count):
        values = from_left(fore, state[f], ((1,), (1,)))
        for tile in range(plan.tiles):
            store_first(plan, out, values[:, tile * LANES : (tile + 1) * LANES], f, count, tile)


def product_kernel(plan, arrived, fore_high, fore_low, back_high, back_low, out):
    fore, back = (fore_high, fore_low), (back_high, back_low)
    for pair in range(plan.tiles // 2):
        grid = []
        for f in range(plan.fields):
            lines = jnp.concatenate([load_first(plan, arrived, f, plan.fields, 2 * pair + h) for h in range(2)], axis=1)
            grid.append(from_left(back, lines))
        u, v, w, b = grid
        square_w = w * w
        products = (u * u - square_w, v * v - square_w, u * v, u * w, v * w, u * b, v * b, w * b)
        for f, product in enumerate(products):
            values = from_left(fore, product)
            for h in range(2):
                store_first(plan, out, values[:, h * LANES : (h + 1) * LANES], f, len(products), 2 * pair + h)


def end_kernel(plan, arrived, back_high, back_low, out):
    back = (back_high, back_low)
    for f in range(plan.fields):
        for pair in range(plan.tiles // 2):
            lines = jnp.concatenate([load_first(plan, arrived, f, plan.fields, 2 * pair + h) for h in range(2)], axis=1)
            values = from_left(back, lines)
            for h in range(2):
                start = (2 * pair + h) * LANES
                out[f, start : start + LANES, :] = values[:, h * LANES : (h + 1) * LANES].T


def first_wave(plan, slot):
    place = lax.axis_index("py") * plan.across_z + lax.axis_index("pz")
    return (place + slot * plan.joint).astype(jnp.float32)


def squared(waves):
    return waves[0] * waves[0] + waves[1] * waves[1] + waves[2] * waves[2]


def project(velocity, waves, shrink):
    along = (waves[0] * velocity[0] + waves[1] * velocity[1] + waves[2] * velocity[2]) * shrink
    return [velocity[i] - waves[i] * along for i in range(3)]


def linear(state, waves, square, shrink):
    pushed = project((coriolis * state[1], -coriolis * state[0], state[3]), waves, shrink)
    return [pushed[i] - viscosity * square * state[i] for i in range(3)] + [
        -buoyancy_square * state[2] - diffusivity * square * state[3]
    ]


def propagate(state, waves, square, shrink):
    for half_step in range(2):
        anchor = state
        for order in (4.0, 3.0, 2.0, 1.0):
            change = linear(state, waves, square, shrink)
            state = [a + (0.5 * time_step / order) * g for a, g in zip(anchor, change)]
    return state


def coarse_setup(plan, slot, wave_y, packed_z):
    waves = (first_wave(plan, slot), wave_y[: plan.coarse_rows, :], packed_z[...])
    square = squared(waves)
    keep = (jnp.abs(waves[1]) <= KCO) & (jnp.abs(waves[2]) <= KCO) & (waves[0] <= KCO)
    return waves, square, 1.0 / jnp.maximum(square, 1.0), keep


def pack(plan, parts):
    lane = lax.broadcasted_iota(jnp.int32, (plan.coarse_rows, LANES), 1)
    real, imag = (part[: plan.coarse_rows] for part in parts)
    return jnp.where(lane < LANES // 2, real, pltpu.roll(imag, LANES // 2, 1))


def start_kernel(plan, arrived, fy_h, fy_l, fz_h, fz_l, by_h, by_l, bz_h, bz_l, wave_y, wave_z, start, out):
    modes = to_waves(plan, arrived, plan.fields, (fy_h, fy_l), (fz_h, fz_l))
    waves = (first_wave(plan, pl.program_id(0)), wave_y[...], wave_z[...])
    shrink = 1.0 / jnp.maximum(squared(waves), 1.0)
    parts = [project([modes[i][c] for i in range(3)], waves, shrink) + [modes[3][c]] for c in range(2)]
    modes = [[parts[c][f] for c in range(2)] for f in range(plan.fields)]
    for f in range(plan.fields):
        for c in range(2):
            start[0, f, c] = modes[f][c]
    send_waves(plan, modes, out, (by_h, by_l), (bz_h, bz_l))


def fine_kernel(plan, count, arrived, start, fy_h, fy_l, fz_h, fz_l, wave_y, wave_z, packed_z, fine, local):
    modes = to_waves(plan, arrived, count, (fy_h, fy_l), (fz_h, fz_l))
    slot = pl.program_id(0)
    waves = (first_wave(plan, slot), wave_y[...], wave_z[...])
    kx, ky, kz = waves
    square = squared(waves)
    shrink = 1.0 / jnp.maximum(square, 1.0)
    before = [[start[0, f, c] for c in range(2)] for f in range(plan.fields)]
    after = [[None, None] for _ in range(plan.fields)]
    for c in range(2):
        sign = 1.0 if c == 0 else -1.0
        uu, vv, uv, uw, vw, ub, vb, wb = (sign * modes[i][1 - c] for i in range(count))
        u, v, w, b = (before[f][c] for f in range(plan.fields))
        pushed = project(
            (
                kx * uu + ky * uv + kz * uw + coriolis * v,
                kx * uv + ky * vv + kz * vw - coriolis * u,
                kx * uw + ky * vw + b,
            ),
            waves,
            shrink,
        )
        rates = [pushed[i] - viscosity * square * (u, v, w)[i] for i in range(3)]
        rates.append(kx * ub + ky * vb + kz * wb - buoyancy_square * w - diffusivity * square * b)
        for f in range(plan.fields):
            after[f][c] = before[f][c] + time_step * rates[f]
            fine[0, f, c] = after[f][c]

    @pl.when(slot < plan.coarse_slots)
    def _():
        coarse, square_c, shrink_c, keep = coarse_setup(plan, slot, wave_y, packed_z)
        moved = propagate([pack(plan, parts) for parts in before], coarse, square_c, shrink_c)
        later = lax.axis_index("tm") > 0
        for f in range(plan.fields):
            less = jnp.where(later, moved[f], 0.0)
            local[0, f] = jnp.where(keep, pack(plan, after[f]) - less, 0.0)


def relay_kernel(plan, arrived, local, wave_y, packed_z, carry):
    coarse, square, shrink, keep = coarse_setup(plan, pl.program_id(0), wave_y, packed_z)
    moved = propagate([arrived[0, f] for f in range(plan.fields)], coarse, square, shrink)
    for f in range(plan.fields):
        carry[0, f] = local[0, f] + jnp.where(keep, moved[f], 0.0)


def merge_kernel(plan, arrived, local, fine, by_h, by_l, bz_h, bz_l, wave_y, packed_z, out):
    coarse, square, shrink, keep = coarse_setup(plan, pl.program_id(0), wave_y, packed_z)
    moved = propagate([arrived[0, f] for f in range(plan.fields)], coarse, square, shrink)
    lane = lax.broadcasted_iota(jnp.int32, (plan.coarse_rows, LANES), 1)
    inside = keep & (lane < LANES // 2)
    modes = []
    for f in range(plan.fields):
        carry = local[0, f] + jnp.where(keep, moved[f], 0.0)
        parts = []
        for c in range(2):
            values = fine[0, f, c]
            own = carry if c == 0 else pltpu.roll(carry, LANES // 2, 1)
            upper = jnp.where(inside, own, values[: plan.coarse_rows])
            parts.append(jnp.concatenate([upper, values[plan.coarse_rows :]], axis=0))
        modes.append(parts)
    send_waves(plan, modes, out, (by_h, by_l), (bz_h, bz_l))


def whole(array):
    return pl.BlockSpec(array.shape, lambda *_: (0,) * array.ndim)


def call(body, plan, name, grid, operands, outputs, **cost):
    def spec(shape, block):
        if block is None:
            return pl.BlockSpec(shape, lambda *_: (0,) * len(shape))
        return pl.BlockSpec(*block)

    shapes = [jax.ShapeDtypeStruct(shape, jnp.float32) for shape, _ in outputs]
    return pl.pallas_call(
        functools.partial(body, plan),
        name=name,
        grid=grid,
        in_specs=[spec(array.shape, block) for array, block in operands],
        out_specs=[spec(shape, block) for shape, block in outputs],
        out_shape=shapes,
        compiler_params=pltpu.CompilerParams(vmem_limit_bytes=VMEM_LIMIT),
    )(*[array for array, _ in operands])


def on_device(state_old):
    plan = Plan(state_old.shape, *(lax.axis_size(axis) for axis in ("tm",) + PAIRS))
    fields, joint, slots, tiles = plan.fields, plan.joint, plan.slots, plan.tiles
    products = 8
    block = 2 * slots * tiles

    def flat(count):
        return (joint * count * block, LANES)

    def split_up(array):
        return array.reshape(joint, -1, block, LANES)

    def exchange(array):
        return lax.all_to_all(array, PAIRS, split_axis=0, concat_axis=0, tiled=True)

    fore_first, back_first = (
        [(jnp.asarray(t), None) for t in split_table(table)] for table in plan.first()
    )
    fore_z, back_z = ([(jnp.asarray(t), None) for t in split_table(table)] for table in plan.along_z())
    fore_y, back_y = ([(jnp.asarray(t), None) for t in split_table(table)] for table in plan.along_y())
    wave_y, wave_z, packed_z = ((jnp.asarray(t), None) for t in plan.wave_tables())

    def sent_block(count):
        return ((joint, count, 2 * tiles, LANES), lambda a: (0, 0, a, 0))

    mode_shape = (slots, fields, 2, plan.wave_rows, LANES)
    mode_block = ((1,) + mode_shape[1:], lambda a: (a, 0, 0, 0, 0))
    coarse_shape = (plan.coarse_slots, fields, plan.coarse_rows, LANES)
    last = plan.coarse_slots - 1
    coarse_block = ((1,) + coarse_shape[1:], lambda a: (jnp.minimum(a, last), 0, 0, 0))

    state = state_old.reshape(fields, plan.rows_y * plan.rows_z, plan.extent)
    (sent,) = call(begin_kernel, plan, "begin", (), [(state, None)] + fore_first, [(flat(fields), None)])
    arrived = exchange(split_up(sent))
    start, sent = call(
        start_kernel,
        plan,
        "start",
        (slots,),
        [(arrived, sent_block(fields))] + fore_y + fore_z + back_y + back_z + [wave_y, wave_z],
        [(mode_shape, mode_block), ((joint, fields, block, LANES), sent_block(fields))],
    )
    arrived = exchange(sent).reshape(flat(fields))
    (sent,) = call(
        product_kernel,
        plan,
        "product",
        (),
        [(arrived, None)] + fore_first + back_first,
        [(flat(products), None)],
    )
    arrived = exchange(split_up(sent))
    fine, local = call(
        lambda plan, *refs: fine_kernel(plan, products, *refs),
        plan,
        "fine",
        (slots,),
        [(arrived, sent_block(products)), (start, mode_block)] + fore_y + fore_z + [wave_y, wave_z, packed_z],
        [(mode_shape, mode_block), (coarse_shape, coarse_block)],
    )
    pairs = [(i, i + 1) for i in range(plan.across_t - 1)]
    received = jnp.zeros_like(local)
    carry = local
    for turn in range(plan.across_t - 1):
        received = lax.ppermute(carry, "tm", pairs)
        if turn < plan.across_t - 2:
            (carry,) = call(
                relay_kernel,
                plan,
                "relay",
                (plan.coarse_slots,),
                [(received, coarse_block), (local, coarse_block), wave_y, packed_z],
                [(coarse_shape, coarse_block)],
            )
    (sent,) = call(
        merge_kernel,
        plan,
        "merge",
        (slots,),
        [(received, coarse_block), (local, coarse_block), (fine, mode_block)]
        + back_y
        + back_z
        + [wave_y, packed_z],
        [((joint, fields, block, LANES), sent_block(fields))],
    )
    arrived = exchange(sent).reshape(flat(fields))
    (out,) = call(end_kernel, plan, "end", (), [(arrived, None)] + back_first, [(state.shape, None)])
    return out.reshape(state_old.shape)


def solution(mesh):
    return jax.shard_map(
        on_device,
        mesh=mesh,
        in_specs=(P("tm", None, "py", "pz", None),),
        out_specs=P("tm", None, "py", "pz", None),
        check_vma=False,
    )
```

```python
import functools

import jax
import jax.numpy as jnp
import numpy as np
from jax import lax
from jax.experimental import pallas as pl
from jax.experimental.pallas import tpu as pltpu
from jax.sharding import PartitionSpec as P

KMAX = 42
KCO = 21

time_step = 0.01
coriolis = 6.0
buoyancy_square = 100.0
viscosity = 0.001
diffusivity = 0.001

LANES = 128
PAIRS = ("py", "pz")
VMEM_LIMIT = 20 * 1024 * 1024


def up_to(value, step):
    return (value + step - 1) // step * step


class Plan:
    def __init__(self, shape, across_t, across_y, across_z):
        _, self.fields, self.rows_y, self.rows_z, self.extent = shape
        self.across_t, self.across_y, self.across_z = across_t, across_y, across_z
        self.joint = across_y * across_z
        self.slots = up_to(KMAX + 1, self.joint) // self.joint
        self.coarse_slots = up_to(KCO + 1, self.joint) // self.joint
        self.group = LANES // self.rows_z
        self.tiles = self.rows_y * self.rows_z // LANES
        self.waves = 2 * KMAX + 1
        self.wave_rows = up_to(self.waves, 8)
        self.coarse_rows = up_to(2 * KCO + 1, 8)
        assert self.extent == LANES and self.extent > 3 * KMAX
        assert self.group == self.across_z and self.tiles == 8
        assert 2 * KCO + 1 <= LANES // 2 <= self.waves <= LANES
        inner = list(range(-KCO, KCO + 1))
        outer = [k for k in range(-KMAX, KMAX + 1) if abs(k) > KCO]
        self.order = np.array(inner + outer)

    def angle(self, waves, cells):
        return 2.0 * np.pi / self.extent * ((waves[:, None] * cells[None, :]) % self.extent)

    def first(self):
        cells = np.arange(self.extent)
        waves = np.arange(self.slots * self.joint)
        inside = (waves <= KMAX)[:, None] * self.extent**-0.5
        weight = np.where(waves == 0, 1.0, 2.0)[:, None] * inside
        angle = self.angle(waves, cells)
        both = np.stack([np.cos(angle), -np.sin(angle)])

        def rows(table):
            table = table.reshape(2, self.slots, self.joint, self.extent)
            return table.transpose(1, 0, 2, 3).reshape(-1, self.extent)

        return rows(both * inside), rows(both * weight).T

    def other(self, size, cells):
        angle = self.angle(self.order, cells)
        cosine = np.zeros((size, len(cells)))
        sine = np.zeros((size, len(cells)))
        cosine[: self.waves] = np.cos(angle) * self.extent**-0.5
        sine[: self.waves] = np.sin(angle) * self.extent**-0.5
        return cosine, sine

    def along_z(self):
        cosine, sine = self.other(LANES, np.arange(self.extent))
        fore = np.block([[cosine.T, -sine.T], [sine.T, cosine.T]])
        back = np.block([[cosine, sine], [-sine, cosine]])
        return fore, back

    def along_y(self):
        cell = np.arange(self.extent).reshape(self.across_y, self.tiles, self.group)
        cosine, sine = self.other(self.wave_rows, cell.transpose(0, 2, 1).reshape(-1))
        fore = np.block([[cosine, sine], [-sine, cosine]])
        back = np.block([[cosine.T, -sine.T], [sine.T, cosine.T]])
        return fore, back

    def wave_tables(self):
        wave_y = np.zeros((self.wave_rows, LANES), np.float32)
        wave_y[: self.waves] = self.order[:, None]
        wave_z = np.zeros((self.wave_rows, LANES), np.float32)
        wave_z[:, : self.waves] = self.order[None, :]
        packed_z = np.tile(self.order[: LANES // 2], 2)
        packed_z = np.broadcast_to(packed_z, (self.coarse_rows, LANES))
        return wave_y, wave_z, packed_z.astype(np.float32)


def split_table(table):
    high = np.asarray(table, np.float32).astype(jnp.bfloat16)
    low = (table - high.astype(np.float64)).astype(np.float32).astype(jnp.bfloat16)
    return high, low


def split(values):
    high = values.astype(jnp.bfloat16)
    low = (values - high.astype(jnp.float32)).astype(jnp.bfloat16)
    return high, low


def dot(left, right, dims=((1,), (0,))):
    return lax.dot_general(left, right, (dims, ((), ())), preferred_element_type=jnp.float32)


def from_left(table, values, dims=((1,), (0,))):
    high, low = split(values)
    table_high, table_low = table[0][...], table[1][...]
    return dot(table_high, high, dims) + (dot(table_high, low, dims) + dot(table_low, high, dims))


def from_right(values, table):
    high, low = split(values)
    table_high, table_low = table[0][...], table[1][...]
    return dot(high, table_high) + (dot(low, table_high) + dot(high, table_low))


def swap_lanes(tiles, width):
    tiles = list(tiles)
    count = len(tiles)
    assert count * width == LANES
    lane = lax.broadcasted_iota(jnp.int32, tiles[0].shape, 1)
    step = count // 2
    while step:
        reach = step * width
        low = (lane // reach) % 2 == 0
        for i in range(count):
            if (i // step) % 2 == 0:
                a, b = tiles[i], tiles[i + step]
                tiles[i] = jnp.where(low, a, pltpu.roll(b, reach, 1))
                tiles[i + step] = jnp.where(low, pltpu.roll(a, LANES - reach, 1), b)
        step //= 2
    return tiles


def arrived_planes(plan, ref, count):
    tiles = plan.tiles
    planes = []
    for f in range(count):
        for c in range(2):
            rows = []
            for p in range(plan.across_y):
                rows.append([ref[p * plan.across_z + q, f, c * tiles : (c + 1) * tiles, :] for q in range(plan.across_z)])
            per_source = [jnp.concatenate([r[q] for r in rows], axis=0) for q in range(plan.across_z)]
            swapped = swap_lanes(per_source, plan.rows_z)
            pieces = []
            for p in range(plan.across_y):
                for g in range(plan.group):
                    pieces.append(swapped[g][p * tiles : (p + 1) * tiles])
            planes.append(jnp.concatenate(pieces, axis=0))
    return planes


def to_waves(plan, ref, count, fore_y, fore_z):
    planes = arrived_planes(plan, ref, count)
    extent = plan.extent
    stacked = jnp.concatenate(
        [jnp.concatenate([planes[2 * f], planes[2 * f + 1]], axis=1) for f in range(count)], axis=0
    )
    along_z = from_right(stacked, fore_z)
    beside = jnp.concatenate(
        [
            jnp.concatenate(
                [along_z[f * extent : (f + 1) * extent, c * LANES : (c + 1) * LANES] for c in range(2)], axis=0
            )
            for f in range(count)
        ],
        axis=1,
    )
    along_y = from_left(fore_y, beside)
    rows = plan.wave_rows
    return [
        [along_y[c * rows : (c + 1) * rows, f * LANES : (f + 1) * LANES] for c in range(2)]
        for f in range(count)
    ]


def send_waves(plan, modes, ref, back_y, back_z):
    count, extent, tiles = len(modes), plan.extent, plan.tiles
    beside = jnp.concatenate([jnp.concatenate(parts, axis=0) for parts in modes], axis=1)
    along_y = from_left(back_y, beside)
    stacked = jnp.concatenate(
        [
            jnp.concatenate(
                [along_y[c * extent : (c + 1) * extent, f * LANES : (f + 1) * LANES] for c in range(2)], axis=1
            )
            for f in range(count)
        ],
        axis=0,
    )
    along_z = from_right(stacked, back_z)
    for f in range(count):
        for c in range(2):
            plane = along_z[f * extent : (f + 1) * extent, c * LANES : (c + 1) * LANES]
            groups = []
            for g in range(plan.group):
                rows = [(p * plan.group + g) * tiles for p in range(plan.across_y)]
                groups.append(jnp.concatenate([plane[r : r + tiles] for r in rows], axis=0))
            swapped = swap_lanes(groups, plan.rows_z)
            for p in range(plan.across_y):
                for q in range(plan.across_z):
                    ref[p * plan.across_z + q, f, c * tiles : (c + 1) * tiles, :] = swapped[q][
                        p * tiles : (p + 1) * tiles
                    ]


def store_first(plan, ref, values, field, count, tile):
    block = 2 * plan.slots * plan.tiles
    for i in range(2 * plan.slots):
        rows = pl.ds(field * block + i * plan.tiles + tile, plan.joint, stride=count * block)
        ref[rows, :] = values[i * plan.joint : (i + 1) * plan.joint]


def load_first(plan, ref, field, count, tile):
    block = 2 * plan.slots * plan.tiles
    return jnp.concatenate(
        [
            ref[pl.ds(field * block + i * plan.tiles + tile, plan.joint, stride=count * block), :]
            for i in range(2 * plan.slots)
        ],
        axis=0,
    )


def begin_kernel(plan, state, fore_high, fore_low, out):
    fore = (fore_high, fore_low)
    count = plan.fields
    for f in range(count):
        values = from_left(fore, state[f], ((1,), (1,)))
        for tile in range(plan.tiles):
            store_first(plan, out, values[:, tile * LANES : (tile + 1) * LANES], f, count, tile)


def product_kernel(plan, arrived, fore_high, fore_low, back_high, back_low, out):
    fore, back = (fore_high, fore_low), (back_high, back_low)
    for pair in range(plan.tiles // 2):
        grid = []
        for f in range(plan.fields):
            lines = jnp.concatenate([load_first(plan, arrived, f, plan.fields, 2 * pair + h) for h in range(2)], axis=1)
            grid.append(from_left(back, lines))
        u, v, w, b = grid
        square_w = w * w
        products = (u * u - square_w, v * v - square_w, u * v, u * w, v * w, u * b, v * b, w * b)
        for f, product in enumerate(products):
            values = from_left(fore, product)
            for h in range(2):
                store_first(plan, out, values[:, h * LANES : (h + 1) * LANES], f, len(products), 2 * pair + h)


def end_kernel(plan, arrived, back_high, back_low, out):
    back = (back_high, back_low)
    for f in range(plan.fields):
        for pair in range(plan.tiles // 2):
            lines = jnp.concatenate([load_first(plan, arrived, f, plan.fields, 2 * pair + h) for h in range(2)], axis=1)
            values = from_left(back, lines)
            for h in range(2):
                start = (2 * pair + h) * LANES
                out[f, start : start + LANES, :] = values[:, h * LANES : (h + 1) * LANES].T


def first_wave(plan, slot):
    place = lax.axis_index("py") * plan.across_z + lax.axis_index("pz")
    return (place + slot * plan.joint).astype(jnp.float32)


def squared(waves):
    return waves[0] * waves[0] + waves[1] * waves[1] + waves[2] * waves[2]


def project(velocity, waves, shrink):
    along = (waves[0] * velocity[0] + waves[1] * velocity[1] + waves[2] * velocity[2]) * shrink
    return [velocity[i] - waves[i] * along for i in range(3)]


def linear(state, waves, square, shrink):
    pushed = project((coriolis * state[1], -coriolis * state[0], state[3]), waves, shrink)
    return [pushed[i] - viscosity * square * state[i] for i in range(3)] + [
        -buoyancy_square * state[2] - diffusivity * square * state[3]
    ]


def propagate(state, waves, square, shrink):
    for half_step in range(2):
        anchor = state
        for order in (4.0, 3.0, 2.0, 1.0):
            change = linear(state, waves, square, shrink)
            state = [a + (0.5 * time_step / order) * g for a, g in zip(anchor, change)]
    return state


def coarse_setup(plan, slot, wave_y, packed_z):
    waves = (first_wave(plan, slot), wave_y[: plan.coarse_rows, :], packed_z[...])
    square = squared(waves)
    keep = (jnp.abs(waves[1]) <= KCO) & (jnp.abs(waves[2]) <= KCO) & (waves[0] <= KCO)
    return waves, square, 1.0 / jnp.maximum(square, 1.0), keep


def pack(plan, parts):
    lane = lax.broadcasted_iota(jnp.int32, (plan.coarse_rows, LANES), 1)
    real, imag = (part[: plan.coarse_rows] for part in parts)
    return jnp.where(lane < LANES // 2, real, pltpu.roll(imag, LANES // 2, 1))


def start_kernel(plan, arrived, fy_h, fy_l, fz_h, fz_l, by_h, by_l, bz_h, bz_l, wave_y, wave_z, start, out):
    modes = to_waves(plan, arrived, plan.fields, (fy_h, fy_l), (fz_h, fz_l))
    waves = (first_wave(plan, pl.program_id(0)), wave_y[...], wave_z[...])
    shrink = 1.0 / jnp.maximum(squared(waves), 1.0)
    parts = [project([modes[i][c] for i in range(3)], waves, shrink) + [modes[3][c]] for c in range(2)]
    modes = [[parts[c][f] for c in range(2)] for f in range(plan.fields)]
    for f in range(plan.fields):
        for c in range(2):
            start[0, f, c] = modes[f][c]
    send_waves(plan, modes, out, (by_h, by_l), (bz_h, bz_l))


def fine_kernel(plan, count, arrived, start, fy_h, fy_l, fz_h, fz_l, wave_y, wave_z, packed_z, fine, local):
    modes = to_waves(plan, arrived, count, (fy_h, fy_l), (fz_h, fz_l))
    slot = pl.program_id(0)
    waves = (first_wave(plan, slot), wave_y[...], wave_z[...])
    kx, ky, kz = waves
    square = squared(waves)
    shrink = 1.0 / jnp.maximum(square, 1.0)
    before = [[start[0, f, c] for c in range(2)] for f in range(plan.fields)]
    after = [[None, None] for _ in range(plan.fields)]
    for c in range(2):
        sign = 1.0 if c == 0 else -1.0
        uu, vv, uv, uw, vw, ub, vb, wb = (sign * modes[i][1 - c] for i in range(count))
        u, v, w, b = (before[f][c] for f in range(plan.fields))
        pushed = project(
            (
                kx * uu + ky * uv + kz * uw + coriolis * v,
                kx * uv + ky * vv + kz * vw - coriolis * u,
                kx * uw + ky * vw + b,
            ),
            waves,
            shrink,
        )
        rates = [pushed[i] - viscosity * square * (u, v, w)[i] for i in range(3)]
        rates.append(kx * ub + ky * vb + kz * wb - buoyancy_square * w - diffusivity * square * b)
        for f in range(plan.fields):
            after[f][c] = before[f][c] + time_step * rates[f]
            fine[0, f, c] = after[f][c]

    @pl.when(slot < plan.coarse_slots)
    def _():
        coarse, square_c, shrink_c, keep = coarse_setup(plan, slot, wave_y, packed_z)
        moved = propagate([pack(plan, parts) for parts in before], coarse, square_c, shrink_c)
        later = lax.axis_index("tm") > 0
        for f in range(plan.fields):
            less = jnp.where(later, moved[f], 0.0)
            local[0, f] = jnp.where(keep, pack(plan, after[f]) - less, 0.0)


def relay_kernel(plan, arrived, local, wave_y, packed_z, carry):
    coarse, square, shrink, keep = coarse_setup(plan, pl.program_id(0), wave_y, packed_z)
    moved = propagate([arrived[0, f] for f in range(plan.fields)], coarse, square, shrink)
    for f in range(plan.fields):
        carry[0, f] = local[0, f] + jnp.where(keep, moved[f], 0.0)


def merge_kernel(plan, arrived, local, fine, by_h, by_l, bz_h, bz_l, wave_y, packed_z, out):
    coarse, square, shrink, keep = coarse_setup(plan, pl.program_id(0), wave_y, packed_z)
    moved = propagate([arrived[0, f] for f in range(plan.fields)], coarse, square, shrink)
    lane = lax.broadcasted_iota(jnp.int32, (plan.coarse_rows, LANES), 1)
    inside = keep & (lane < LANES // 2)
    modes = []
    for f in range(plan.fields):
        carry = local[0, f] + jnp.where(keep, moved[f], 0.0)
        parts = []
        for c in range(2):
            values = fine[0, f, c]
            own = carry if c == 0 else pltpu.roll(carry, LANES // 2, 1)
            upper = jnp.where(inside, own, values[: plan.coarse_rows])
            parts.append(jnp.concatenate([upper, values[plan.coarse_rows :]], axis=0))
        modes.append(parts)
    send_waves(plan, modes, out, (by_h, by_l), (bz_h, bz_l))


def whole(array):
    return pl.BlockSpec(array.shape, lambda *_: (0,) * array.ndim)


def call(body, plan, name, grid, operands, outputs, **cost):
    def spec(shape, block):
        if block is None:
            return pl.BlockSpec(shape, lambda *_: (0,) * len(shape))
        return pl.BlockSpec(*block)

    shapes = [jax.ShapeDtypeStruct(shape, jnp.float32) for shape, _ in outputs]
    return pl.pallas_call(
        functools.partial(body, plan),
        name=name,
        grid=grid,
        in_specs=[spec(array.shape, block) for array, block in operands],
        out_specs=[spec(shape, block) for shape, block in outputs],
        out_shape=shapes,
        compiler_params=pltpu.CompilerParams(vmem_limit_bytes=VMEM_LIMIT),
    )(*[array for array, _ in operands])


def on_device(state_old):
    plan = Plan(state_old.shape, *(lax.axis_size(axis) for axis in ("tm",) + PAIRS))
    fields, joint, slots, tiles = plan.fields, plan.joint, plan.slots, plan.tiles
    products = 8
    block = 2 * slots * tiles

    def flat(count):
        return (joint * count * block, LANES)

    def split_up(array):
        return array.reshape(joint, -1, block, LANES)

    def exchange(array):
        return lax.all_to_all(array, PAIRS, split_axis=0, concat_axis=0, tiled=True)

    fore_first, back_first = (
        [(jnp.asarray(t), None) for t in split_table(table)] for table in plan.first()
    )
    fore_z, back_z = ([(jnp.asarray(t), None) for t in split_table(table)] for table in plan.along_z())
    fore_y, back_y = ([(jnp.asarray(t), None) for t in split_table(table)] for table in plan.along_y())
    wave_y, wave_z, packed_z = ((jnp.asarray(t), None) for t in plan.wave_tables())

    def sent_block(count):
        return ((joint, count, 2 * tiles, LANES), lambda a: (0, 0, a, 0))

    mode_shape = (slots, fields, 2, plan.wave_rows, LANES)
    mode_block = ((1,) + mode_shape[1:], lambda a: (a, 0, 0, 0, 0))
    coarse_shape = (plan.coarse_slots, fields, plan.coarse_rows, LANES)
    last = plan.coarse_slots - 1
    coarse_block = ((1,) + coarse_shape[1:], lambda a: (jnp.minimum(a, last), 0, 0, 0))

    state = state_old.reshape(fields, plan.rows_y * plan.rows_z, plan.extent)
    (sent,) = call(begin_kernel, plan, "begin", (), [(state, None)] + fore_first, [(flat(fields), None)])
    arrived = exchange(split_up(sent))
    start, sent = call(
        start_kernel,
        plan,
        "start",
        (slots,),
        [(arrived, sent_block(fields))] + fore_y + fore_z + back_y + back_z + [wave_y, wave_z],
        [(mode_shape, mode_block), ((joint, fields, block, LANES), sent_block(fields))],
    )
    arrived = exchange(sent).reshape(flat(fields))
    (sent,) = call(
        product_kernel,
        plan,
        "product",
        (),
        [(arrived, None)] + fore_first + back_first,
        [(flat(products), None)],
    )
    arrived = exchange(split_up(sent))
    fine, local = call(
        lambda plan, *refs: fine_kernel(plan, products, *refs),
        plan,
        "fine",
        (slots,),
        [(arrived, sent_block(products)), (start, mode_block)] + fore_y + fore_z + [wave_y, wave_z, packed_z],
        [(mode_shape, mode_block), (coarse_shape, coarse_block)],
    )
    pairs = [(i, i + 1) for i in range(plan.across_t - 1)]
    received = jnp.zeros_like(local)
    carry = local
    for turn in range(plan.across_t - 1):
        received = lax.ppermute(carry, "tm", pairs)
        if turn < plan.across_t - 2:
            (carry,) = call(
                relay_kernel,
                plan,
                "relay",
                (plan.coarse_slots,),
                [(received, coarse_block), (local, coarse_block), wave_y, packed_z],
                [(coarse_shape, coarse_block)],
            )
    (sent,) = call(
        merge_kernel,
        plan,
        "merge",
        (slots,),
        [(received, coarse_block), (local, coarse_block), (fine, mode_block)]
        + back_y
        + back_z
        + [wave_y, packed_z],
        [((joint, fields, block, LANES), sent_block(fields))],
    )
    arrived = exchange(sent).reshape(flat(fields))
    (out,) = call(end_kernel, plan, "end", (), [(arrived, None)] + back_first, [(state.shape, None)])
    return out.reshape(state_old.shape)


def solution(mesh):
    return jax.shard_map(
        on_device,
        mesh=mesh,
        in_specs=(P("tm", None, "py", "pz", None),),
        out_specs=P("tm", None, "py", "pz", None),
        check_vma=False,
    )
```

```python
import functools

import jax
import jax.numpy as jnp
import numpy as np
from jax import lax
from jax.experimental import pallas as pl
from jax.experimental.pallas import tpu as pltpu
from jax.sharding import PartitionSpec as P

KMAX = 42
KCO = 21

time_step = 0.01
coriolis = 6.0
buoyancy_square = 100.0
viscosity = 0.001
diffusivity = 0.001

LANES = 128
PAIRS = ("py", "pz")
VMEM_LIMIT = 20 * 1024 * 1024
FLOPS_PER_MICRO = 6e8
PRODUCTS = 8


def up_to(value, step):
    return (value + step - 1) // step * step


class Plan:
    def __init__(self, shape, across_t, across_y, across_z):
        _, self.fields, self.rows_y, self.rows_z, self.extent = shape
        self.across_t, self.across_y, self.across_z = across_t, across_y, across_z
        self.joint = across_y * across_z
        self.slots = up_to(KMAX + 1, self.joint) // self.joint
        self.coarse_slots = up_to(KCO + 1, self.joint) // self.joint
        self.group = LANES // self.rows_z
        self.tiles = self.rows_y * self.rows_z // LANES
        self.waves = 2 * KMAX + 1
        self.wave_rows = up_to(self.waves, 8)
        self.coarse_rows = up_to(2 * KCO + 1, 8)
        self.lines = 2 * across_y
        self.chunks = [(slot,) for slot in range(self.slots)]
        assert self.extent == LANES and self.extent > 3 * KMAX
        assert self.group == across_z == across_y == self.fields and self.tiles == 8
        assert self.lines == 8 and LANES // self.rows_y == across_y
        assert across_y & (across_y - 1) == 0
        assert 2 * KCO + 1 <= LANES // 2 <= self.waves <= LANES
        inner = list(range(-KCO, KCO + 1))
        outer = [k for k in range(-KMAX, KMAX + 1) if abs(k) > KCO]
        self.order = np.array(inner + outer)

    def angle(self, waves, cells):
        return 2.0 * np.pi / self.extent * ((waves[:, None] * cells[None, :]) % self.extent)

    def first(self):
        cells = np.arange(self.extent)
        waves = np.arange(self.slots * self.joint)
        inside = (waves <= KMAX)[:, None] * self.extent**-0.5
        weight = np.where(waves == 0, 1.0, 2.0)[:, None] * inside
        angle = self.angle(waves, cells)
        both = np.stack([np.cos(angle), -np.sin(angle)])

        def arranged(table):
            table = table.reshape(2, self.slots, self.across_y, self.across_z, self.extent)
            return table.transpose(1, 0, 2, 3, 4)

        return arranged(both * inside), arranged(both * weight)

    def other(self, size, cells):
        angle = self.angle(self.order, cells)
        cosine = np.zeros((size, len(cells)))
        sine = np.zeros((size, len(cells)))
        cosine[: self.waves] = np.cos(angle) * self.extent**-0.5
        sine[: self.waves] = np.sin(angle) * self.extent**-0.5
        return cosine, sine

    def along_z(self):
        cosine, sine = self.other(self.wave_rows, np.arange(self.extent))
        fore = np.block([[cosine, sine], [-sine, cosine]])
        back = np.block([[cosine, sine], [-sine, cosine]])
        return fore, back

    def along_y(self):
        cell = np.arange(self.extent).reshape(self.across_y, self.tiles, self.group)
        cosine, sine = self.other(LANES, cell.transpose(0, 2, 1).reshape(-1))
        fore = np.block([[cosine.T, -sine.T], [sine.T, cosine.T]])
        back = np.block([[cosine, sine], [-sine, cosine]])
        return fore, back

    def wave_tables(self):
        wave_z = np.zeros((self.wave_rows, LANES), np.float32)
        wave_z[: self.waves] = self.order[:, None]
        wave_y = np.zeros((self.wave_rows, LANES), np.float32)
        wave_y[:, : self.waves] = self.order[None, :]
        packed_y = np.tile(self.order[: LANES // 2], 2)
        packed_y = np.broadcast_to(packed_y, (self.coarse_rows, LANES))
        return wave_y, wave_z, packed_y.astype(np.float32)


def exchanged(table, axis, place, count):
    bits = count.bit_length() - 1
    shape = table.shape
    table = table.reshape(shape[:axis] + (2,) * bits + shape[axis + 1 :])
    for bit in range(bits):
        here = axis + bits - 1 - bit
        table = jnp.where((place >> bit) % 2 == 1, jnp.flip(table, here), table)
    return table.reshape(shape)


def split_table(table):
    high = np.asarray(table, np.float32).astype(jnp.bfloat16)
    low = (table - high.astype(np.float64)).astype(np.float32).astype(jnp.bfloat16)
    return high, low


def split(values):
    high = values.astype(jnp.bfloat16)
    low = (values - high.astype(jnp.float32)).astype(jnp.bfloat16)
    return high, low


def dot(left, right, dims=((1,), (0,))):
    return lax.dot_general(left, right, (dims, ((), ())), preferred_element_type=jnp.float32)


def from_left(table, values, dims=((1,), (0,))):
    high, low = split(values)
    table_high, table_low = table[0][...], table[1][...]
    return dot(table_high, high, dims) + (dot(table_high, low, dims) + dot(table_low, high, dims))


def from_right(values, table):
    high, low = split(values)
    table_high, table_low = table[0][...], table[1][...]
    return dot(high, table_high) + (dot(low, table_high) + dot(high, table_low))


def swap_lanes(tiles, width):
    tiles = list(tiles)
    count = len(tiles)
    assert count * width == LANES
    lane = lax.broadcasted_iota(jnp.int32, tiles[0].shape, 1)
    step = count // 2
    while step:
        reach = step * width
        low = (lane // reach) % 2 == 0
        for i in range(count):
            if (i // step) % 2 == 0:
                a, b = tiles[i], tiles[i + step]
                tiles[i] = jnp.where(low, a, pltpu.roll(b, reach, 1))
                tiles[i + step] = jnp.where(low, pltpu.roll(a, LANES - reach, 1), b)
        step //= 2
    return tiles


def to_planes(plan, refs, count, size, ai, line):
    tiles = []
    for ref in refs:
        tiles.append(jnp.concatenate([ref[f, ai, line] for f in range(count)], axis=0))
    swapped = swap_lanes(tiles, plan.rows_z)
    step = plan.tiles
    planes = []
    for h in range(count // plan.fields):
        pieces = []
        for f in range(h * plan.fields, (h + 1) * plan.fields):
            pieces += [swapped[g][f * step : (f + 1) * step] for g in range(plan.group)]
        planes.append(jnp.concatenate(pieces, axis=0))
    return planes


def fore_z_kernel(plan, count, size, *refs):
    q, p = plan.across_z, plan.across_y
    arrived, (table_h, table_l), outs = refs[:q], refs[q : q + 2], refs[q + 2 :]
    for ai in range(size):
        for h in range(count // plan.fields):
            stacked = []
            for m in range(p):
                parts = [to_planes(plan, arrived, count, size, ai, c * p + m)[h] for c in range(2)]
                stacked.append(jnp.concatenate(parts, axis=1))
            values = from_left((table_h, table_l), jnp.concatenate(stacked, axis=0), ((1,), (1,)))
            for m in range(p):
                outs[m][ai, h] = values[:, m * LANES : (m + 1) * LANES]


def back_z_kernel(plan, size, *refs):
    p, q = plan.across_y, plan.across_z
    arrived, (table_h, table_l), outs = refs[:p], refs[p : p + 2], refs[p + 2 :]
    rows, step = plan.rows_y, plan.tiles
    for ai in range(size):
        stacked = jnp.concatenate([arrived[m][ai, 0].T for m in range(p)], axis=0)
        values = from_right(stacked, (table_h, table_l))
        for c in range(2):
            groups = []
            for g in range(plan.group):
                pieces = []
                for m in range(p):
                    for f in range(plan.fields):
                        start = m * LANES + f * rows + g * step
                        pieces.append(values[start : start + step, c * LANES : (c + 1) * LANES])
                groups.append(jnp.concatenate(pieces, axis=0))
            swapped = swap_lanes(groups, plan.rows_z)
            for k in range(q):
                for m in range(p):
                    for f in range(plan.fields):
                        start = (m * plan.fields + f) * step
                        outs[k][f, ai, c * p + m] = swapped[k][start : start + step]


def to_waves(plan, refs, count, ai, fore_y):
    rows = plan.wave_rows
    stacked = []
    for h in range(count // plan.fields):
        swapped = swap_lanes([ref[ai, h] for ref in refs], plan.rows_y)
        stacked += [jnp.concatenate([s[:rows], s[rows:]], axis=1) for s in swapped]
    values = from_right(jnp.concatenate(stacked, axis=0), fore_y)
    return [
        [values[f * rows : (f + 1) * rows, c * LANES : (c + 1) * LANES] for c in range(2)]
        for f in range(count)
    ]


def send_waves(plan, modes, outs, ai, back_y):
    rows = plan.wave_rows
    stacked = jnp.concatenate([jnp.concatenate(parts, axis=1) for parts in modes], axis=0)
    values = from_right(stacked, back_y)
    tiles = []
    for f in range(len(modes)):
        own = values[f * rows : (f + 1) * rows]
        tiles.append(jnp.concatenate([own[:, :LANES], own[:, LANES:]], axis=0))
    swapped = swap_lanes(tiles, plan.rows_y)
    for m in range(plan.across_y):
        outs[m][ai, 0] = swapped[m]


def tile_rows(plan, size, field, ai, tile):
    block = plan.lines * plan.tiles
    return pl.ds((field * size + ai) * block + tile, plan.lines, stride=plan.tiles)


def store_first(plan, outs, values, field, tile):
    for n, chunk in enumerate(plan.chunks):
        for k in range(plan.across_z):
            for ai, a in enumerate(chunk):
                start = (k * plan.slots + a) * plan.lines
                out = outs[n * plan.across_z + k]
                out[tile_rows(plan, len(chunk), field, ai, tile), :] = values[start : start + plan.lines]


def load_first(plan, refs, field, tile):
    pieces = []
    for k in range(plan.across_z):
        for n, chunk in enumerate(plan.chunks):
            for ai in range(len(chunk)):
                ref = refs[n * plan.across_z + k]
                pieces.append(ref[tile_rows(plan, len(chunk), field, ai, tile), :])
    return jnp.concatenate(pieces, axis=0)


def begin_kernel(plan, state, fore_high, fore_low, *outs):
    fore = (fore_high, fore_low)
    for f in range(plan.fields):
        values = from_left(fore, state[f], ((1,), (1,)))
        for tile in range(plan.tiles):
            store_first(plan, outs, values[:, tile * LANES : (tile + 1) * LANES], f, tile)


def grid_values(plan, arrived, back, field, pair):
    lines = [load_first(plan, arrived, field, 2 * pair + h) for h in range(2)]
    return from_left(back, jnp.concatenate(lines, axis=1))


def product_kernel(plan, *refs):
    count = len(plan.chunks) * plan.across_z
    arrived, (fore_h, fore_l, back_h, back_l), outs = refs[:count], refs[count : count + 4], refs[count + 4 :]
    for pair in range(plan.tiles // 2):
        u, v, w, b = (grid_values(plan, arrived, (back_h, back_l), f, pair) for f in range(plan.fields))
        square_w = w * w
        products = (u * u - square_w, v * v - square_w, u * v, u * w, v * w, u * b, v * b, w * b)
        for f, product in enumerate(products):
            values = from_left((fore_h, fore_l), product)
            for h in range(2):
                store_first(plan, outs, values[:, h * LANES : (h + 1) * LANES], f, 2 * pair + h)


def end_kernel(plan, *refs):
    arrived, (back_h, back_l, out) = refs[:-3], refs[-3:]
    for f in range(plan.fields):
        for pair in range(plan.tiles // 2):
            values = grid_values(plan, arrived, (back_h, back_l), f, pair)
            for h in range(2):
                start = (2 * pair + h) * LANES
                out[f, start : start + LANES, :] = values[:, h * LANES : (h + 1) * LANES].T


def first_wave(plan, slot):
    place = lax.axis_index("py") * plan.across_z + lax.axis_index("pz")
    return (place + slot * plan.joint).astype(jnp.float32)


def squared(waves):
    return waves[0] * waves[0] + waves[1] * waves[1] + waves[2] * waves[2]


def project(velocity, waves, shrink):
    along = (waves[0] * velocity[0] + waves[1] * velocity[1] + waves[2] * velocity[2]) * shrink
    return [velocity[i] - waves[i] * along for i in range(3)]


def linear(state, waves, square, shrink):
    pushed = project((coriolis * state[1], -coriolis * state[0], state[3]), waves, shrink)
    return [pushed[i] - viscosity * square * state[i] for i in range(3)] + [
        -buoyancy_square * state[2] - diffusivity * square * state[3]
    ]


def propagate(state, waves, square, shrink):
    for half_step in range(2):
        anchor = state
        for order in (4.0, 3.0, 2.0, 1.0):
            change = linear(state, waves, square, shrink)
            state = [a + (0.5 * time_step / order) * g for a, g in zip(anchor, change)]
    return state


def coarse_setup(plan, slot, packed_y, wave_z):
    waves = (first_wave(plan, slot), packed_y[...], wave_z[: plan.coarse_rows, :])
    square = squared(waves)
    keep = (jnp.abs(waves[1]) <= KCO) & (jnp.abs(waves[2]) <= KCO) & (waves[0] <= KCO)
    return waves, square, 1.0 / jnp.maximum(square, 1.0), keep


def pack(plan, parts):
    lane = lax.broadcasted_iota(jnp.int32, (plan.coarse_rows, LANES), 1)
    real, imag = (part[: plan.coarse_rows] for part in parts)
    return jnp.where(lane < LANES // 2, real, pltpu.roll(imag, LANES // 2, 1))


def start_kernel(plan, chunk, *refs):
    p = plan.across_y
    arrived, (fy_h, fy_l, by_h, by_l, wave_y, wave_z, start), outs = refs[:p], refs[p : p + 7], refs[p + 7 :]
    for ai, slot in enumerate(chunk):
        modes = to_waves(plan, arrived, plan.fields, ai, (fy_h, fy_l))
        waves = (first_wave(plan, slot), wave_y[...], wave_z[...])
        shrink = 1.0 / jnp.maximum(squared(waves), 1.0)
        parts = [project([modes[i][c] for i in range(3)], waves, shrink) + [modes[3][c]] for c in range(2)]
        modes = [[parts[c][f] for c in range(2)] for f in range(plan.fields)]
        for f in range(plan.fields):
            for c in range(2):
                start[ai, f, c] = modes[f][c]
        send_waves(plan, modes, outs, ai, (by_h, by_l))


def finer(plan, slot, modes, before, waves):
    kx, ky, kz = waves
    square = squared(waves)
    shrink = 1.0 / jnp.maximum(square, 1.0)
    after = [[None, None] for _ in range(plan.fields)]
    for c in range(2):
        sign = 1.0 if c == 0 else -1.0
        uu, vv, uv, uw, vw, ub, vb, wb = (sign * mode[1 - c] for mode in modes)
        u, v, w, b = (before[f][c] for f in range(plan.fields))
        pushed = project(
            (
                kx * uu + ky * uv + kz * uw + coriolis * v,
                kx * uv + ky * vv + kz * vw - coriolis * u,
                kx * uw + ky * vw + b,
            ),
            waves,
            shrink,
        )
        rates = [pushed[i] - viscosity * square * (u, v, w)[i] for i in range(3)]
        rates.append(kx * ub + ky * vb + kz * wb - buoyancy_square * w - diffusivity * square * b)
        for f in range(plan.fields):
            after[f][c] = before[f][c] + time_step * rates[f]
    return after


def fine_kernel(plan, chunk, *refs):
    p = plan.across_y
    arrived, (start, fy_h, fy_l, wave_y, wave_z, packed_y, fine, local) = refs[:p], refs[p:]
    later = lax.axis_index("tm") > 0
    for ai, slot in enumerate(chunk):
        modes = to_waves(plan, arrived, PRODUCTS, ai, (fy_h, fy_l))
        waves = (first_wave(plan, slot), wave_y[...], wave_z[...])
        before = [[start[ai, f, c] for c in range(2)] for f in range(plan.fields)]
        after = finer(plan, slot, modes, before, waves)
        for f in range(plan.fields):
            for c in range(2):
                fine[ai, f, c] = after[f][c]
        coarse, square, shrink, keep = coarse_setup(plan, slot, packed_y, wave_z)
        moved = propagate([pack(plan, parts) for parts in before], coarse, square, shrink)
        for f in range(plan.fields):
            less = jnp.where(later, moved[f], 0.0)
            local[ai, f] = jnp.where(keep, pack(plan, after[f]) - less, 0.0)


def fine_send_kernel(plan, chunk, *refs):
    p = plan.across_y
    arrived, (start, fy_h, fy_l, by_h, by_l, wave_y, wave_z), outs = refs[:p], refs[p : p + 7], refs[p + 7 :]
    for ai, slot in enumerate(chunk):
        modes = to_waves(plan, arrived, PRODUCTS, ai, (fy_h, fy_l))
        waves = (first_wave(plan, slot), wave_y[...], wave_z[...])
        before = [[start[ai, f, c] for c in range(2)] for f in range(plan.fields)]
        after = finer(plan, slot, modes, before, waves)
        send_waves(plan, after, outs, ai, (by_h, by_l))


def relay_kernel(plan, chunk, arrived, local, wave_z, packed_y, carry):
    for ai, slot in enumerate(chunk):
        coarse, square, shrink, keep = coarse_setup(plan, slot, packed_y, wave_z)
        moved = propagate([arrived[ai, f] for f in range(plan.fields)], coarse, square, shrink)
        for f in range(plan.fields):
            carry[ai, f] = local[ai, f] + jnp.where(keep, moved[f], 0.0)


def merge_kernel(plan, chunk, arrived, local, fine, by_h, by_l, wave_z, packed_y, *outs):
    lane = lax.broadcasted_iota(jnp.int32, (plan.coarse_rows, LANES), 1)
    for ai, slot in enumerate(chunk):
        coarse, square, shrink, keep = coarse_setup(plan, slot, packed_y, wave_z)
        moved = propagate([arrived[ai, f] for f in range(plan.fields)], coarse, square, shrink)
        inside = keep & (lane < LANES // 2)
        modes = []
        for f in range(plan.fields):
            carry = local[ai, f] + jnp.where(keep, moved[f], 0.0)
            parts = []
            for c in range(2):
                values = fine[ai, f, c]
                own = carry if c == 0 else pltpu.roll(carry, LANES // 2, 1)
                upper = jnp.where(inside, own, values[: plan.coarse_rows])
                parts.append(jnp.concatenate([upper, values[plan.coarse_rows :]], axis=0))
            modes.append(parts)
        send_waves(plan, modes, outs, ai, (by_h, by_l))


def call(body, name, micros, operands, shapes, after=()):
    spec = lambda shape: pl.BlockSpec(shape, lambda *_: (0,) * len(shape))
    count, skip = len(operands), len(operands) + len(after)
    operands = operands + list(after)
    return pl.pallas_call(
        lambda *refs: body(*refs[:count], *refs[skip:]),
        name=name,
        in_specs=[spec(array.shape) for array in operands[:count]]
        + [pl.BlockSpec(memory_space=pl.ANY) for _ in after],
        out_specs=[spec(shape) for shape in shapes],
        out_shape=[jax.ShapeDtypeStruct(shape, jnp.float32) for shape in shapes],
        compiler_params=pltpu.CompilerParams(vmem_limit_bytes=VMEM_LIMIT),
        cost_estimate=pl.CostEstimate(
            flops=int(micros * FLOPS_PER_MICRO), bytes_accessed=1 << 20, transcendentals=0
        ),
    )(*operands)


def on_device(state_old):
    plan = Plan(state_old.shape, *(lax.axis_size(axis) for axis in ("tm",) + PAIRS))
    fields, tiles, lines = plan.fields, plan.tiles, plan.lines
    p, q = plan.across_y, plan.across_z
    place_p, place_q = (lax.axis_index(axis) for axis in PAIRS)

    def swapped(arrays, axis):
        pairs = lambda k: [(i, i ^ k) for i in range(len(arrays))]
        return [a if k == 0 else lax.ppermute(a, axis, pairs(k)) for k, a in enumerate(arrays)]

    first = np.stack([t for table in plan.first() for t in split_table(table)])
    first = exchanged(exchanged(jnp.asarray(first), 3, place_p, p), 4, place_q, q)
    first = first.transpose(0, 4, 1, 2, 3, 5).reshape(4, -1, plan.extent)
    fore_first, back_first = [first[0], first[1]], [first[2].T, first[3].T]

    def placed(table, axis, place, count):
        parts = []
        for t in split_table(table):
            shape = t.shape
            t = t.reshape(shape[:axis] + (2, count, shape[axis] // 2 // count) + shape[axis + 1 :])
            t = exchanged(jnp.asarray(t), axis + 1, place, count)
            parts.append(t.reshape(shape))
        return parts

    fore_z, back_z = (placed(table, 1, place_q, q) for table in plan.along_z())
    fore_y, back_y = plan.along_y()
    fore_y, back_y = placed(fore_y, 0, place_p, p), placed(back_y, 1, place_p, p)
    wave_y, wave_z, packed_y = (jnp.asarray(t) for t in plan.wave_tables())

    def first_shapes(count):
        return [(count * len(chunk) * lines * tiles, LANES) for chunk in plan.chunks for _ in range(q)]

    def by_lines(arrays, count, size):
        return [a.reshape(count, size, lines, tiles, LANES) for a in arrays]

    def flat(arrays):
        return [a.reshape(-1, LANES) for a in arrays]

    def second_shapes(count, size):
        return [(size, count // fields, 2 * plan.wave_rows, LANES)] * p

    def to_lines(arrays, chunk, count, after):
        size = len(chunk)
        arrived = by_lines(swapped(arrays, "pz"), count, size)
        sent = call(
            functools.partial(fore_z_kernel, plan, count, size),
            "fore_z",
            0.2 * size * count,
            arrived + fore_z,
            second_shapes(count, size),
            after,
        )
        return sent

    def from_lines(sent, chunk, after):
        size = len(chunk)
        arrived = swapped(sent, "py")
        sent = call(
            functools.partial(back_z_kernel, plan, size),
            "back_z",
            0.8 * size,
            arrived + back_z,
            [(fields, size, lines, tiles, LANES)] * q,
            after,
        )
        return sent

    def mode_shape(chunk):
        return (len(chunk), fields, 2, plan.wave_rows, LANES)

    def coarse_shape(chunk):
        return (len(chunk), fields, plan.coarse_rows, LANES)

    state = state_old.reshape(fields, plan.rows_y * plan.rows_z, plan.extent)
    sent = call(functools.partial(begin_kernel, plan), "begin", 2.0, [state] + fore_first, first_shapes(fields))
    def all_lines(sent, count):
        result, after = [], []
        for n, chunk in enumerate(plan.chunks):
            result.append(to_lines(sent[n * q : (n + 1) * q], chunk, count, after))
            after = result[-1][:1]
        return result, after

    def all_tiles(sent, after):
        result = []
        for chunk, back in zip(plan.chunks, sent):
            result.append(from_lines(back, chunk, after))
            after = result[-1][:1]
        return [a for tiles in result for a in flat(swapped(tiles, "pz"))]

    lined, after = all_lines(sent, fields)
    starts, backs = [], []
    for n, chunk in enumerate(plan.chunks):
        start, *back = call(
            functools.partial(start_kernel, plan, chunk),
            "start",
            1.0 * len(chunk),
            swapped(lined[n], "py") + fore_y + back_y + [wave_y, wave_z],
            [mode_shape(chunk)] + second_shapes(fields, len(chunk)),
            after,
        )
        starts.append(start)
        backs.append(back)
        after = [start]
    arrived = all_tiles(backs, after)
    sent = call(
        functools.partial(product_kernel, plan),
        "product",
        3.0,
        arrived + fore_first + back_first,
        first_shapes(PRODUCTS),
    )
    pairs = [(i, i + 1) for i in range(plan.across_t - 1)]
    lined, after = all_lines(sent, PRODUCTS)
    backs, held = [None] * len(plan.chunks), []
    coarse = [n for n, chunk in enumerate(plan.chunks) if chunk[0] < plan.coarse_slots]
    for n, chunk in enumerate(plan.chunks):
        lines_y = swapped(lined[n], "py")
        if n in coarse:
            fine, local = call(
                functools.partial(fine_kernel, plan, chunk),
                "fine",
                1.0 * len(chunk),
                lines_y + [starts[n]] + fore_y + [wave_y, wave_z, packed_y],
                [mode_shape(chunk), coarse_shape(chunk)],
                after,
            )
            after = [local]
            held.append((fine, local))
        if n == coarse[-1]:
            for m, (fine, local) in zip(coarse, held):
                chunk_m = plan.chunks[m]
                received, carry = jnp.zeros_like(local), local
                for turn in range(plan.across_t - 1):
                    received = lax.ppermute(carry, "tm", pairs)
                    if turn < plan.across_t - 2:
                        (carry,) = call(
                            functools.partial(relay_kernel, plan, chunk_m),
                            "relay",
                            1.0,
                            [received, local, wave_z, packed_y],
                            [coarse_shape(chunk_m)],
                        )
                backs[m] = call(
                    functools.partial(merge_kernel, plan, chunk_m),
                    "merge",
                    0.7 * len(chunk_m),
                    [received, local, fine] + back_y + [wave_z, packed_y],
                    second_shapes(fields, len(chunk_m)),
                    after,
                )
                after = backs[m][:1]
        if n not in coarse:
            backs[n] = call(
                functools.partial(fine_send_kernel, plan, chunk),
                "fine_send",
                1.3 * len(chunk),
                lines_y + [starts[n]] + fore_y + back_y + [wave_y, wave_z],
                second_shapes(fields, len(chunk)),
                after,
            )
            after = backs[n][:1]
    arrived = all_tiles(backs, after)
    (out,) = call(functools.partial(end_kernel, plan), "end", 3.0, arrived + back_first, [state.shape])
    return out.reshape(state_old.shape)


def solution(mesh):
    return jax.shard_map(
        on_device,
        mesh=mesh,
        in_specs=(P("tm", None, "py", "pz", None),),
        out_specs=P("tm", None, "py", "pz", None),
        check_vma=False,
    )
```

```python
import functools

import jax
import jax.numpy as jnp
import numpy as np
from jax import lax
from jax.experimental import pallas as pl
from jax.experimental.pallas import tpu as pltpu
from jax.sharding import PartitionSpec as P


KMAX = 42
KCO = 21

time_step = 0.01
coriolis = 6.0
buoyancy_square = 100.0
viscosity = 0.001
diffusivity = 0.001

LANES = 128
PAIRS = ("py", "pz")
VMEM_LIMIT = 20 * 1024 * 1024
FLOPS_PER_MICRO = 6e8
PRODUCTS = 8


def up_to(value, step):
    return (value + step - 1) // step * step


class Plan:
    def __init__(self, shape, across_t, across_y, across_z):
        _, self.fields, self.rows_y, self.rows_z, self.extent = shape
        self.across_t, self.across_y, self.across_z = across_t, across_y, across_z
        self.joint = across_y * across_z
        self.slots = up_to(KMAX + 1, self.joint) // self.joint
        self.coarse_slots = up_to(KCO + 1, self.joint) // self.joint
        self.group = LANES // self.rows_z
        self.tiles = self.rows_y * self.rows_z // LANES
        self.waves = 2 * KMAX + 1
        self.wave_rows = up_to(self.waves, 8)
        self.coarse_rows = up_to(2 * KCO + 1, 8)
        self.lines = 2 * across_y
        self.chunks = [(slot,) for slot in range(self.slots)]
        spread = lambda i: ((i // across_z % 2) * 2 + i % 2) * (self.joint // 4) + (
            i // across_z // 2 * (across_z // 2) + i % across_z // 2
        )
        self.ranks = [spread(i) for i in range(self.joint)]
        assert sorted(self.ranks) == list(range(self.joint))
        assert self.extent == LANES and self.extent > 3 * KMAX
        assert self.group == across_z == across_y == self.fields and self.tiles == 8
        assert self.lines == 8 and LANES // self.rows_y == across_y
        assert across_y & (across_y - 1) == 0
        assert 2 * KCO + 1 <= LANES // 2 <= self.waves <= LANES
        inner = list(range(-KCO, KCO + 1))
        outer = [k for k in range(-KMAX, KMAX + 1) if abs(k) > KCO]
        self.order = np.array(inner + outer)

    def holds(self, chunk, place, most):
        return any(a * self.joint + self.ranks[place] <= most for a in chunk)

    def rank(self, place_p, place_q):
        inner = (place_p % 2) * 2 + place_q % 2
        return inner * (self.joint // 4) + place_p // 2 * (self.across_z // 2) + place_q // 2

    def angle(self, waves, cells):
        return 2.0 * np.pi / self.extent * ((waves[:, None] * cells[None, :]) % self.extent)

    def first(self):
        cells = np.arange(self.extent)
        waves = np.arange(self.slots)[:, None] * self.joint + np.array(self.ranks)[None, :]
        waves = waves.reshape(-1)
        inside = (waves <= KMAX)[:, None] * self.extent**-0.5
        weight = np.where(waves == 0, 1.0, 2.0)[:, None] * inside
        angle = self.angle(waves, cells)
        both = np.stack([np.cos(angle), -np.sin(angle)])

        def arranged(table):
            table = table.reshape(2, self.slots, self.across_y, self.across_z, self.extent)
            return table.transpose(3, 1, 0, 2, 4).reshape(-1, self.extent).astype(np.float32)

        return arranged(both * inside), arranged(both * weight)

    def other(self, size, cells):
        angle = self.angle(self.order, cells)
        cosine = np.zeros((size, len(cells)))
        sine = np.zeros((size, len(cells)))
        cosine[: self.waves] = np.cos(angle) * self.extent**-0.5
        sine[: self.waves] = np.sin(angle) * self.extent**-0.5
        return cosine, sine

    def along_z(self):
        cosine, sine = self.other(self.wave_rows, np.arange(self.extent))
        fore = np.block([[cosine, sine], [-sine, cosine]])
        back = np.block([[cosine, sine], [-sine, cosine]])
        return fore, back

    def along_y(self):
        cell = np.arange(self.extent).reshape(self.across_y, self.tiles, self.group)
        cosine, sine = self.other(LANES, cell.transpose(0, 2, 1).reshape(-1))
        fore = np.block([[cosine, sine], [-sine, cosine]])
        back = np.block([[cosine, sine], [-sine, cosine]])
        return fore, back

    def wave_tables(self):
        wave_z = np.zeros((self.wave_rows, LANES), np.float32)
        wave_z[: self.waves] = self.order[:, None]
        wave_y = np.zeros((self.wave_rows, LANES), np.float32)
        wave_y[:, : self.waves] = self.order[None, :]
        packed_y = np.tile(self.order[: LANES // 2], 2)
        packed_y = np.broadcast_to(packed_y, (self.coarse_rows, LANES))
        return wave_y, wave_z, packed_y.astype(np.float32)


def split(values):
    high = values.astype(jnp.bfloat16)
    low = (values - high.astype(jnp.float32)).astype(jnp.bfloat16)
    return high, low


def dot(left, right, dims=((1,), (0,))):
    return lax.dot_general(left, right, (dims, ((), ())), preferred_element_type=jnp.float32)


def from_left(table, values, dims=((1,), (0,))):
    high, low = split(values)
    table_high, table_low = table[0][...], table[1][...]
    return dot(table_high, high, dims) + (dot(table_high, low, dims) + dot(table_low, high, dims))


def from_right(values, table, dims=((1,), (0,))):
    high, low = split(values)
    table_high, table_low = table[0][...], table[1][...]
    return dot(high, table_high, dims) + (dot(low, table_high, dims) + dot(high, table_low, dims))


def flipped(values, axis, reach, place, bit):
    size = values.shape[axis]
    low = (lax.broadcasted_iota(jnp.int32, values.shape, axis) // reach) % 2 == 0
    other = jnp.where(low, pltpu.roll(values, size - reach, axis), pltpu.roll(values, reach, axis))
    return jnp.where((place >> bit) % 2 == 1, other, values)


def relative_first(plan, ref):
    place_p, place_q = lax.axis_index("py"), lax.axis_index("pz")
    size = plan.slots * plan.lines
    blocks = [
        ref[pl.ds(pl.multiple_of((place_q ^ k) * size, 8), size), :] for k in range(plan.across_z)
    ]
    table = jnp.concatenate(blocks, axis=0)
    for bit in range(plan.across_y.bit_length() - 1):
        table = flipped(table, 0, 1 << bit, place_p, bit)
    return table


def tables_kernel(plan, *refs):
    count = len(refs) // 3
    for n in range(count):
        axis, width, blocks = (
            ("pz", plan.rows_z, plan.across_z) if n < 2 else ("py", plan.rows_y, plan.across_y)
        )
        place = lax.axis_index(axis)
        for c in range(2):
            lanes = slice(c * LANES, (c + 1) * LANES)
            table = refs[n][:, lanes]
            for bit in range(blocks.bit_length() - 1):
                table = flipped(table, 1, width << bit, place, bit)
            high, low = split(table)
            refs[count + 2 * n][:, lanes] = high
            refs[count + 2 * n + 1][:, lanes] = low


def swap_lanes(tiles, width):
    tiles = list(tiles)
    count = len(tiles)
    assert count * width == LANES
    lane = lax.broadcasted_iota(jnp.int32, tiles[0].shape, 1)
    step = count // 2
    while step:
        reach = step * width
        low = (lane // reach) % 2 == 0
        for i in range(count):
            if (i // step) % 2 == 0:
                a, b = tiles[i], tiles[i + step]
                tiles[i] = jnp.where(low, a, pltpu.roll(b, reach, 1))
                tiles[i + step] = jnp.where(low, pltpu.roll(a, LANES - reach, 1), b)
        step //= 2
    return tiles


def to_planes(plan, refs, count, ai, line):
    tiles = []
    for ref in refs:
        tiles.append(jnp.concatenate([ref[f, ai, line] for f in range(count)], axis=0))
    swapped = swap_lanes(tiles, plan.rows_z)
    step = plan.tiles
    planes = []
    for h in range(count // plan.fields):
        pieces = []
        for f in range(h * plan.fields, (h + 1) * plan.fields):
            pieces += [swapped[g][f * step : (f + 1) * step] for g in range(plan.group)]
        planes.append(jnp.concatenate(pieces, axis=0))
    return planes


def combined(plan, first, second, wave_x, wave_z):
    rows = plan.wave_rows
    place = lax.broadcasted_iota(jnp.int32, (rows, LANES), 1) // plan.rows_y
    even, one = place % 2 == 0, place == 1
    of_first = jnp.where(even, wave_x, jnp.where(one, wave_z, 1.0))
    of_second = jnp.where(even, wave_z, jnp.where(one, wave_x, 0.0))
    pieces = []
    for c in range(2):
        a, b = first[c * rows : (c + 1) * rows], second[c * rows : (c + 1) * rows]
        pieces.append(of_first * a + of_second * jnp.where(one, pltpu.roll(b, plan.rows_y, 1), b))
    pieces.append(jnp.where(even, pltpu.roll(second[rows:], LANES - plan.rows_y, 1), second[:rows]))
    return jnp.concatenate(pieces, axis=0)


def fore_z_kernel(plan, count, chunk, *refs):
    q, p = plan.across_z, plan.across_y
    arrived, (table_h, table_l, wave_z), outs = refs[:q], refs[q : q + 3], refs[q + 3 :]
    place_p, place_q = lax.axis_index("py"), lax.axis_index("pz")
    for ai, slot in enumerate(chunk):
        planes = [to_planes(plan, arrived, count, ai, line) for line in range(2 * p)]
        values = []
        for h in range(count // plan.fields):
            stacked = [jnp.concatenate([planes[m][h], planes[p + m][h]], axis=1) for m in range(p)]
            values.append(from_left((table_h, table_l), jnp.concatenate(stacked, axis=0), ((1,), (1,))))
        for m in range(p):
            own = [v[:, m * LANES : (m + 1) * LANES] for v in values]
            if count == plan.fields:
                outs[m][ai] = own[0]
            else:
                wave_x = plan.rank(place_p ^ m, place_q) + slot * plan.joint
                outs[m][ai] = combined(plan, own[0], own[1], wave_x.astype(jnp.float32), wave_z[...])


def back_z_kernel(plan, size, *refs):
    p, q = plan.across_y, plan.across_z
    arrived, (table_h, table_l), outs = refs[:p], refs[p : p + 2], refs[p + 2 :]
    rows, step = plan.rows_y, plan.tiles
    for ai in range(size):
        stacked = jnp.concatenate([arrived[m][ai].T for m in range(p)], axis=0)
        values = from_right(stacked, (table_h, table_l))
        for c in range(2):
            groups = []
            for g in range(plan.group):
                pieces = []
                for m in range(p):
                    for f in range(plan.fields):
                        start = m * LANES + f * rows + g * step
                        pieces.append(values[start : start + step, c * LANES : (c + 1) * LANES])
                groups.append(jnp.concatenate(pieces, axis=0))
            swapped = swap_lanes(groups, plan.rows_z)
            for k in range(q):
                for m in range(p):
                    for f in range(plan.fields):
                        start = (m * plan.fields + f) * step
                        outs[k][f, ai, c * p + m] = swapped[k][start : start + step]


def to_waves(plan, refs, count, ai, fore_y):
    rows = plan.wave_rows
    swapped = swap_lanes([ref[ai] for ref in refs], plan.rows_y)
    pairs = [(s[:rows], s[rows : 2 * rows]) for s in swapped]
    if count > plan.fields:
        last = [s[2 * rows :] for s in swapped]
        pairs += [(last[1], last[0]), (last[3], last[2])]
    stacked = jnp.concatenate([jnp.concatenate(pair, axis=1) for pair in pairs], axis=0)
    values = from_right(stacked, fore_y, ((1,), (1,)))
    return [
        [values[f * rows : (f + 1) * rows, c * LANES : (c + 1) * LANES] for c in range(2)]
        for f in range(len(pairs))
    ]


def send_waves(plan, modes, outs, ai, back_y):
    rows = plan.wave_rows
    stacked = jnp.concatenate([jnp.concatenate(parts, axis=1) for parts in modes], axis=0)
    values = from_right(stacked, back_y)
    tiles = []
    for f in range(len(modes)):
        own = values[f * rows : (f + 1) * rows]
        tiles.append(jnp.concatenate([own[:, :LANES], own[:, LANES:]], axis=0))
    swapped = swap_lanes(tiles, plan.rows_y)
    for m in range(plan.across_y):
        outs[m][ai] = swapped[m]


def tile_rows(plan, size, field, ai, tile):
    block = plan.lines * plan.tiles
    return pl.ds((field * size + ai) * block + tile, plan.lines, stride=plan.tiles)


def store_first(plan, outs, values, field, tile):
    for n, chunk in enumerate(plan.chunks):
        for k in range(plan.across_z):
            for ai, a in enumerate(chunk):
                start = (k * plan.slots + a) * plan.lines
                out = outs[n * plan.across_z + k]
                out[tile_rows(plan, len(chunk), field, ai, tile), :] = values[start : start + plan.lines]


def load_first(plan, refs, field, tile):
    pieces = []
    for k in range(plan.across_z):
        for n, chunk in enumerate(plan.chunks):
            for ai in range(len(chunk)):
                ref = refs[n * plan.across_z + k]
                pieces.append(ref[tile_rows(plan, len(chunk), field, ai, tile), :])
    return jnp.concatenate(pieces, axis=0)


def begin_kernel(plan, state, fore_first, *outs):
    fore = split(relative_first(plan, fore_first))
    for f in range(plan.fields):
        values = from_left(fore, state[f], ((1,), (1,)))
        for tile in range(plan.tiles):
            store_first(plan, outs, values[:, tile * LANES : (tile + 1) * LANES], f, tile)


def grid_values(plan, arrived, back, field, pair):
    lines = [load_first(plan, arrived, field, 2 * pair + h) for h in range(2)]
    return from_left(back, jnp.concatenate(lines, axis=1))


def product_kernel(plan, *refs):
    count = len(plan.chunks) * plan.across_z
    arrived, (fore_first, back_first), outs = refs[:count], refs[count : count + 2], refs[count + 2 :]
    fore = split(relative_first(plan, fore_first))
    back = split(relative_first(plan, back_first).T)
    for pair in range(plan.tiles // 2):
        u, v, w, b = (grid_values(plan, arrived, back, f, pair) for f in range(plan.fields))
        square_v = v * v
        products = (u * u - square_v, w * w - square_v, u * b, u * v, u * w, v * w, w * b, v * b)
        for f, product in enumerate(products):
            values = from_left(fore, product)
            for h in range(2):
                store_first(plan, outs, values[:, h * LANES : (h + 1) * LANES], f, 2 * pair + h)


def end_kernel(plan, *refs):
    arrived, (back_first, out) = refs[:-2], refs[-2:]
    back = split(relative_first(plan, back_first).T)
    for f in range(plan.fields):
        for pair in range(plan.tiles // 2):
            values = grid_values(plan, arrived, back, f, pair)
            for h in range(2):
                start = (2 * pair + h) * LANES
                out[f, start : start + LANES, :] = values[:, h * LANES : (h + 1) * LANES].T


def first_wave(plan, slot):
    rank = plan.rank(lax.axis_index("py"), lax.axis_index("pz"))
    return (rank + slot * plan.joint).astype(jnp.float32)


def squared(waves):
    return waves[0] * waves[0] + waves[1] * waves[1] + waves[2] * waves[2]


def project(velocity, waves, shrink):
    along = (waves[0] * velocity[0] + waves[1] * velocity[1] + waves[2] * velocity[2]) * shrink
    return [velocity[i] - waves[i] * along for i in range(3)]


def linear(state, waves, square, shrink):
    pushed = project((coriolis * state[1], -coriolis * state[0], state[3]), waves, shrink)
    return [pushed[i] - viscosity * square * state[i] for i in range(3)] + [
        -buoyancy_square * state[2] - diffusivity * square * state[3]
    ]


def propagate(state, waves, square, shrink):
    for _ in range(2):
        anchor = state
        for order in (4.0, 3.0, 2.0, 1.0):
            change = linear(state, waves, square, shrink)
            state = [a + (0.5 * time_step / order) * g for a, g in zip(anchor, change)]
    return state


def coarse_setup(plan, slot, packed_y, wave_z):
    waves = (first_wave(plan, slot), packed_y[...], wave_z[: plan.coarse_rows, :])
    square = squared(waves)
    keep = (jnp.abs(waves[1]) <= KCO) & (jnp.abs(waves[2]) <= KCO) & (waves[0] <= KCO)
    return waves, square, 1.0 / jnp.maximum(square, 1.0), keep


def pack(plan, parts):
    lane = lax.broadcasted_iota(jnp.int32, (plan.coarse_rows, LANES), 1)
    real, imag = (part[: plan.coarse_rows] for part in parts)
    return jnp.where(lane < LANES // 2, real, pltpu.roll(imag, LANES // 2, 1))


def start_kernel(plan, chunk, *refs):
    p = plan.across_y
    arrived, (fy_h, fy_l, by_h, by_l, wave_y, wave_z, start), outs = refs[:p], refs[p : p + 7], refs[p + 7 :]
    for ai, slot in enumerate(chunk):
        modes = to_waves(plan, arrived, plan.fields, ai, (fy_h, fy_l))
        waves = (first_wave(plan, slot), wave_y[...], wave_z[...])
        shrink = 1.0 / jnp.maximum(squared(waves), 1.0)
        parts = [project([modes[i][c] for i in range(3)], waves, shrink) + [modes[3][c]] for c in range(2)]
        modes = [[parts[c][f] for c in range(2)] for f in range(plan.fields)]
        for f in range(plan.fields):
            for c in range(2):
                start[ai, f, c] = modes[f][c]
        send_waves(plan, modes, outs, ai, (by_h, by_l))


def finer(plan, modes, before, waves):
    kx, ky, kz = waves
    square = squared(waves)
    shrink = 1.0 / jnp.maximum(square, 1.0)
    after = [[None, None] for _ in range(plan.fields)]
    for c in range(2):
        sign = 1.0 if c == 0 else -1.0
        cross_1, cross_3, flux, uv, vw, vb = (sign * mode[1 - c] for mode in modes)
        u, v, w, b = (before[f][c] for f in range(plan.fields))
        pushed = project(
            (
                cross_1 + ky * uv + coriolis * v,
                kx * uv + kz * vw - coriolis * u,
                cross_3 + ky * vw + b,
            ),
            waves,
            shrink,
        )
        rates = [pushed[i] - viscosity * square * (u, v, w)[i] for i in range(3)]
        rates.append(flux + ky * vb - buoyancy_square * w - diffusivity * square * b)
        for f in range(plan.fields):
            after[f][c] = before[f][c] + time_step * rates[f]
    return after


def fine_kernel(plan, chunk, *refs):
    p = plan.across_y
    arrived, (start, fy_h, fy_l, wave_y, wave_z, packed_y, fine, local) = refs[:p], refs[p:]
    later = lax.axis_index("tm") > 0
    for ai, slot in enumerate(chunk):
        modes = to_waves(plan, arrived, PRODUCTS, ai, (fy_h, fy_l))
        waves = (first_wave(plan, slot), wave_y[...], wave_z[...])
        before = [[start[ai, f, c] for c in range(2)] for f in range(plan.fields)]
        after = finer(plan, modes, before, waves)
        for f in range(plan.fields):
            for c in range(2):
                fine[ai, f, c] = after[f][c]
        coarse, square, shrink, keep = coarse_setup(plan, slot, packed_y, wave_z)
        moved = propagate([pack(plan, parts) for parts in before], coarse, square, shrink)
        for f in range(plan.fields):
            less = jnp.where(later, moved[f], 0.0)
            local[ai, f] = jnp.where(keep, pack(plan, after[f]) - less, 0.0)


def fine_send_kernel(plan, chunk, *refs):
    p = plan.across_y
    arrived, (start, fy_h, fy_l, by_h, by_l, wave_y, wave_z), outs = refs[:p], refs[p : p + 7], refs[p + 7 :]
    for ai, slot in enumerate(chunk):
        modes = to_waves(plan, arrived, PRODUCTS, ai, (fy_h, fy_l))
        waves = (first_wave(plan, slot), wave_y[...], wave_z[...])
        before = [[start[ai, f, c] for c in range(2)] for f in range(plan.fields)]
        after = finer(plan, modes, before, waves)
        send_waves(plan, after, outs, ai, (by_h, by_l))


def relay_kernel(plan, chunk, arrived, local, wave_z, packed_y, carry):
    for ai, slot in enumerate(chunk):
        coarse, square, shrink, keep = coarse_setup(plan, slot, packed_y, wave_z)
        moved = propagate([arrived[ai, f] for f in range(plan.fields)], coarse, square, shrink)
        for f in range(plan.fields):
            carry[ai, f] = local[ai, f] + jnp.where(keep, moved[f], 0.0)


def merge_kernel(plan, chunk, arrived, local, fine, by_h, by_l, wave_z, packed_y, *outs):
    lane = lax.broadcasted_iota(jnp.int32, (plan.coarse_rows, LANES), 1)
    for ai, slot in enumerate(chunk):
        coarse, square, shrink, keep = coarse_setup(plan, slot, packed_y, wave_z)
        moved = propagate([arrived[ai, f] for f in range(plan.fields)], coarse, square, shrink)
        inside = keep & (lane < LANES // 2)
        modes = []
        for f in range(plan.fields):
            carry = local[ai, f] + jnp.where(keep, moved[f], 0.0)
            parts = []
            for c in range(2):
                values = fine[ai, f, c]
                own = carry if c == 0 else pltpu.roll(carry, LANES // 2, 1)
                upper = jnp.where(inside, own, values[: plan.coarse_rows])
                parts.append(jnp.concatenate([upper, values[plan.coarse_rows :]], axis=0))
            modes.append(parts)
        send_waves(plan, modes, outs, ai, (by_h, by_l))


def call(body, micros, operands, shapes, after=(), dtype=jnp.float32):
    spec = lambda shape: pl.BlockSpec(shape, lambda *_: (0,) * len(shape))
    count, skip = len(operands), len(operands) + len(after)
    operands = operands + list(after)
    return pl.pallas_call(
        lambda *refs: body(*refs[:count], *refs[skip:]),
        in_specs=[spec(array.shape) for array in operands[:count]]
        + [pl.BlockSpec(memory_space=pl.ANY) for _ in after],
        out_specs=[spec(shape) for shape in shapes],
        out_shape=[jax.ShapeDtypeStruct(shape, dtype) for shape in shapes],
        compiler_params=pltpu.CompilerParams(vmem_limit_bytes=VMEM_LIMIT),
        cost_estimate=pl.CostEstimate(
            flops=int(micros * FLOPS_PER_MICRO), bytes_accessed=1 << 20, transcendentals=0
        ),
    )(*operands)


def on_device(state_old):
    plan = Plan(state_old.shape, *(lax.axis_size(axis) for axis in ("tm",) + PAIRS))
    fields, tiles, lines = plan.fields, plan.tiles, plan.lines
    p, q = plan.across_y, plan.across_z

    def swapped(arrays):
        pairs = lambda k: [(i, i ^ k) for i in range(q)]
        return [a if k == 0 else lax.ppermute(a, "pz", pairs(k)) for k, a in enumerate(arrays)]

    def gathered(arrays):
        pairs = lambda m: [(i, i ^ m) for i in range(p)]
        return [a if m == 0 else lax.ppermute(a, "py", pairs(m)) for m, a in enumerate(arrays)]

    def returned(arrays):
        pairs = lambda m: [(i, i ^ m) for i in range(p)]
        return [a if m == 0 else lax.ppermute(a, "py", pairs(m)) for m, a in enumerate(arrays)]

    fore_first, back_first = (jnp.asarray(table) for table in plan.first())
    wave_y, wave_z, packed_y = (jnp.asarray(t) for t in plan.wave_tables())

    def first_shapes(count):
        return [(count * len(chunk) * lines * tiles, LANES) for chunk in plan.chunks for _ in range(q)]

    def by_lines(arrays, count, size):
        return [a.reshape(count, size, lines, tiles, LANES) for a in arrays]

    def flat(arrays):
        return [a.reshape(-1, LANES) for a in arrays]

    def second_shapes(count, size):
        return [(size, (2 if count == fields else 3) * plan.wave_rows, LANES)] * p

    def to_lines(arrays, chunk, count, after):
        size = len(chunk)
        arrived = by_lines(swapped(arrays), count, size)
        sent = call(
            functools.partial(fore_z_kernel, plan, count, chunk),
            0.2 * size * count,
            arrived + fore_z + [wave_z],
            second_shapes(count, size),
            after,
        )
        return sent

    def from_lines(sent, chunk, after):
        size = len(chunk)
        arrived = returned(sent)
        sent = call(
            functools.partial(back_z_kernel, plan, size),
            0.8 * size,
            arrived + back_z,
            [(fields, size, lines, tiles, LANES)] * q,
            after,
        )
        return sent

    def mode_shape(chunk):
        return (len(chunk), fields, 2, plan.wave_rows, LANES)

    def coarse_shape(chunk):
        return (len(chunk), fields, plan.coarse_rows, LANES)

    state = state_old.reshape(fields, plan.rows_y * plan.rows_z, plan.extent)
    sent = call(functools.partial(begin_kernel, plan), 2.0, [state, fore_first], first_shapes(fields))
    plain = [jnp.asarray(t, jnp.float32) for t in plan.along_z() + plan.along_y()]
    tables = call(
        functools.partial(tables_kernel, plan),
        1.0,
        plain,
        [t.shape for t in plain for _ in range(2)],
        sent[:1],
        jnp.bfloat16,
    )
    fore_z, back_z, fore_y, back_y = (list(tables[2 * n : 2 * n + 2]) for n in range(4))

    def all_lines(sent, count):
        result, after = [], []
        for n, chunk in enumerate(plan.chunks):
            result.append(to_lines(sent[n * q : (n + 1) * q], chunk, count, after))
            after = result[-1][:1]
        return result, after

    def all_tiles(sent, after):
        result = []
        for chunk, back in zip(plan.chunks, sent):
            result.append(from_lines(back, chunk, after))
            after = result[-1][:1]
        return [a for tiles in result for a in flat(swapped(tiles))]

    lined, after = all_lines(sent, fields)
    starts, backs = [], []
    for n, chunk in enumerate(plan.chunks):
        start, *back = call(
            functools.partial(start_kernel, plan, chunk),
            1.0 * len(chunk),
            gathered(lined[n]) + fore_y + back_y + [wave_y, wave_z],
            [mode_shape(chunk)] + second_shapes(fields, len(chunk)),
            after,
        )
        starts.append(start)
        backs.append(back)
        after = [start]
    arrived = all_tiles(backs, after)
    sent = call(
        functools.partial(product_kernel, plan),
        3.0,
        arrived + [fore_first, back_first],
        first_shapes(PRODUCTS),
    )
    lined, backs, held = {}, {}, {}
    after = []
    coarse = [n for n, chunk in enumerate(plan.chunks) if chunk[0] < plan.coarse_slots]

    def fore(n, after):
        lined[n] = to_lines(sent[n * q : (n + 1) * q], plan.chunks[n], PRODUCTS, after)
        return lined[n][:1]

    def refine(n, after):
        chunk = plan.chunks[n]
        held[n] = call(
            functools.partial(fine_kernel, plan, chunk),
            1.0 * len(chunk),
            gathered(lined[n]) + [starts[n]] + fore_y + [wave_y, wave_z, packed_y],
            [mode_shape(chunk), coarse_shape(chunk)],
            after,
        )
        return held[n][1:]

    def merge(n, after):
        chunk, (fine, local) = plan.chunks[n], held[n]
        pairs = [
            (t * p * q + i, (t + 1) * p * q + i)
            for t in range(plan.across_t - 1)
            for i in range(p * q)
            if plan.holds(chunk, i, KCO)
        ]
        received, carry = jnp.zeros_like(local), local
        for turn in range(plan.across_t - 1):
            received = lax.ppermute(carry, ("tm",) + PAIRS, pairs)
            if turn < plan.across_t - 2:
                (carry,) = call(
                    functools.partial(relay_kernel, plan, chunk),
                    1.0,
                    [received, local, wave_z, packed_y],
                    [coarse_shape(chunk)],
                )
        backs[n] = call(
            functools.partial(merge_kernel, plan, chunk),
            0.7 * len(chunk),
            [received, local, fine] + back_y + [wave_z, packed_y],
            second_shapes(fields, len(chunk)),
            after,
        )
        return backs[n][:1]

    def refine_and_send(n, after):
        chunk = plan.chunks[n]
        backs[n] = call(
            functools.partial(fine_send_kernel, plan, chunk),
            1.3 * len(chunk),
            gathered(lined[n]) + [starts[n]] + fore_y + back_y + [wave_y, wave_z],
            second_shapes(fields, len(chunk)),
            after,
        )
        return backs[n][:1]

    steps = {"fore_z": fore, "fine": refine, "merge": merge, "send": refine_and_send}
    for step, n in second_half(len(plan.chunks), len(coarse)):
        after = steps[step](n, after)
    backs = [backs[n] for n in range(len(plan.chunks))]
    arrived = all_tiles(backs, after)
    (out,) = call(functools.partial(end_kernel, plan), 3.0, arrived + [back_first], [state.shape])
    return out.reshape(state_old.shape)


def second_half(slots, coarse):
    chain = [("fore_z", n) for n in range(slots)]
    chain.insert(2, ("fine", 0))
    chain += [("merge", 0)]
    for n in range(1, coarse):
        chain += [("fine", n), ("merge", n)]
    return chain + [("send", n) for n in range(coarse, slots)]


def solution(mesh):
    return jax.shard_map(
        on_device,
        mesh=mesh,
        in_specs=(P("tm", None, "py", "pz", None),),
        out_specs=P("tm", None, "py", "pz", None),
        check_vma=False,
    )
```
